512 devices in a mesh: head: 8 (over y_hi, core), blk: 64 (over z, y_lo, x).
Axes of the slice: x: 4, y: 8 (y_hi: 4, y_lo: 2; y = y_hi * 2 + y_lo), z: 8, core: 2. Of those that a mesh axis runs over, the one named last changes fastest.
Arguments:
- query_rows: bfloat16 [64, 144, 3072], P('blk', 'head'), may hold values from -6 to 6
- key_rows: bfloat16 [64, 144, 3072], P('blk', 'head'), may hold values from -6 to 6
- value_rows: bfloat16 [64, 144, 3072], P('blk', 'head'), may hold values from -6 to 6
- query_tangent: bfloat16 [64, 144, 3072], P('blk', 'head'), may hold values from -6 to 6
- key_tangent: bfloat16 [64, 144, 3072], P('blk', 'head'), may hold values from -6 to 6
- value_tangent: bfloat16 [64, 144, 3072], P('blk', 'head'), may hold values from -6 to 6
- query_gain: float32 [128], replicated, may hold values from 1 to 6
- key_gain: float32 [128], replicated, may hold values from 1 to 6
Outputs:
- attended: bfloat16 [64, 144, 3072], P('blk', 'head')
- attended_tangent: bfloat16 [64, 144, 3072], P('blk', 'head')
The draws below stay inside these ranges and needn't reach their ends.
All inputs are finite; a program needn't handle non-finite values.
Results may differ from the reference program's by a relative error of at most 0.014.
The reference program's roundings to bfloat16 on the way count: a program that leaves them out, or rounds other values in their place, can miss the bound.
Values may be sent and summed in bfloat16 or wider, within the bound.
A program may use at most 64 MiB of HBM per device.

```python
import math
import jax
import jax.numpy as jnp
from jax import lax

HEADS = 24
HD = 128
D = 3072
TXT = 512
GRID_W = 64
GROUP = 16
ROWS = 144
IMAGES = 4
SEQ = 2304
BLOCKS = 64


def joint_pair(key):
    shape = (IMAGES, SEQ, D)
    key_values = jax.random.normal(jax.random.fold_in(key, 101), shape, jnp.float32)
    query_values = jax.random.normal(jax.random.fold_in(key, 102), shape, jnp.float32)

    def blocked(feature_field):
        feature_field = jnp.clip(feature_field, -6.0, 6.0).reshape(IMAGES, GROUP, ROWS, D)
        return feature_field.transpose(1, 0, 2, 3).reshape(GROUP * IMAGES, ROWS, D).astype(jnp.bfloat16)
    return (blocked(query_values), blocked(key_values))


def gain_draw(key):
    return jnp.exp(jax.random.uniform(key, (HD,), jnp.float32, 0.0, jnp.log(2.2)))


def draw_query_rows(key, part):
    return joint_pair(key)[0]


def draw_key_rows(key, part):
    return joint_pair(key)[1]


def draw_query_gain(key, part):
    return gain_draw(jax.random.fold_in(key, 201))


def draw_key_gain(key, part):
    return gain_draw(jax.random.fold_in(key, 202))


def level_of(own_key, extent, shards, least, top_value):
    factor_of = 1.0
    for dim, blocks in shards:
        heights = jax.random.uniform(jax.random.fold_in(jax.random.fold_in(own_key, 6), dim), (blocks,), jnp.float32, least / len(shards), top_value / len(shards))
        factor_of = factor_of * jnp.repeat(jnp.exp(heights), extent[dim] // blocks).reshape((-1,) + (1,) * (len(extent) - 1 - dim))
    return factor_of


def normal_values(own_key, dims, spread, bound, shards=(), held_as=jnp.bfloat16):
    loudness = level_of(own_key, dims, shards, -0.22, 0.18) if shards else 1.0
    values = jax.random.normal(own_key, dims, jnp.float32) * spread * loudness
    return jnp.minimum(jnp.maximum(values, -bound), bound).astype(held_as)


def setup_inputs(seed: int = 0) -> dict:
    key_of = jax.random.split(jax.random.key(seed), 9)
    query_rows = draw_query_rows(jax.random.fold_in(key_of[8], 71), 0)
    key_rows = draw_key_rows(jax.random.fold_in(key_of[8], 71), 0)
    value_rows = normal_values(key_of[2], (BLOCKS, ROWS, D), 1.0, 6.0, ((0, 64), (1, 8)))
    query_tangent = normal_values(key_of[3], (BLOCKS, ROWS, D), 1.0, 6.0, ((0, 64), (1, 8)))
    key_tangent = normal_values(key_of[4], (BLOCKS, ROWS, D), 1.0, 6.0, ((0, 64), (1, 8)))
    value_tangent = normal_values(key_of[5], (BLOCKS, ROWS, D), 1.0, 6.0, ((0, 64), (1, 8)))
    query_gain = draw_query_gain(jax.random.fold_in(key_of[8], 71), 0)
    key_gain = draw_key_gain(jax.random.fold_in(key_of[8], 71), 0)
    return {"query_rows": query_rows, "key_rows": key_rows, "value_rows": value_rows, "query_tangent": query_tangent, "key_tangent": key_tangent, "value_tangent": value_tangent, "query_gain": query_gain, "key_gain": key_gain}


EPSILON = 1e-06
THETA = 10000.0

def rotation(first, count, head_dim):
    block_offsets = first + jnp.arange(count, dtype=jnp.int32)
    is_image = block_offsets >= TXT
    patch = jnp.maximum(block_offsets - TXT, 0)
    row_id = jnp.where(is_image, patch // GRID_W, 0).astype(jnp.float32)
    column_id = jnp.where(is_image, patch % GRID_W, 0).astype(jnp.float32)
    leading = head_dim // 8
    lateral = (head_dim - leading) // 2
    exponent = jnp.arange(lateral // 2, dtype=jnp.float32) * (2.0 / lateral)
    frequency = jnp.exp(-math.log(THETA) * exponent)
    angles = jnp.concatenate([jnp.zeros((count, leading // 2), jnp.float32), row_id[:, None] * frequency[None, :], column_id[:, None] * frequency[None, :]], axis=1)
    angles = jnp.repeat(angles, 2, axis=1)
    return (jnp.cos(angles), jnp.sin(angles))

def rotation_partner(head_dim):
    across = jnp.arange(head_dim, dtype=jnp.int32)
    lower = across[:, None]
    upper = across[None, :]
    forward = ((upper == lower + 1) & (lower % 2 == 0)).astype(jnp.float32)
    backward = ((lower == upper + 1) & (upper % 2 == 0)).astype(jnp.float32)
    return forward - backward

def normalize(raw, tangent, gain, cosine, sine, partner):
    values = raw.astype(jnp.float32)
    motion = tangent.astype(jnp.float32)
    inverse = lax.rsqrt(lax.optimization_barrier(jnp.mean(values * values, axis=-1, keepdims=True)) + EPSILON)
    coupling = lax.optimization_barrier(jnp.mean(values * motion, axis=-1, keepdims=True))
    normed = values * inverse * gain
    normalized_tangent = gain * (motion * inverse - values * inverse * inverse * inverse * coupling)

    def rotate(feature_field):
        return feature_field * cosine + jnp.dot(feature_field, partner, precision=lax.Precision.HIGHEST) * sine
    return (rotate(normed).astype(jnp.bfloat16), rotate(normalized_tangent).astype(jnp.bfloat16))

def attend(item):
    query_hat, query_dot, key_hat, key_dot, value, value_dot = [feature_field.astype(jnp.float32) for feature_field in item]
    scale = 1.0 / math.sqrt(HD)
    logit_scores = jnp.dot(query_hat, key_hat.T, preferred_element_type=jnp.float32) * scale
    peak = lax.optimization_barrier(jnp.max(logit_scores, axis=1, keepdims=True))
    weights = jnp.exp(logit_scores - peak)
    total = lax.optimization_barrier(jnp.sum(weights, axis=1, keepdims=True))
    score_dot = (jnp.dot(query_dot, key_hat.T, preferred_element_type=jnp.float32) + jnp.dot(query_hat, key_dot.T, preferred_element_type=jnp.float32)) * scale
    product = weights * score_dot
    drift = lax.optimization_barrier(jnp.sum(product, axis=1, keepdims=True))
    low_weights = lax.optimization_barrier(weights.astype(jnp.bfloat16)).astype(jnp.float32)
    low_product = lax.optimization_barrier(product.astype(jnp.bfloat16)).astype(jnp.float32)
    summed = jnp.dot(low_weights, value, preferred_element_type=jnp.float32)
    summed_dot = jnp.dot(low_weights, value_dot, preferred_element_type=jnp.float32) + jnp.dot(low_product, value, preferred_element_type=jnp.float32)
    attention_output = (summed / total).astype(jnp.bfloat16)
    output_tangent = ((summed_dot - drift / total * summed) / total).astype(jnp.bfloat16)
    return (attention_output, output_tangent)

def reference(query_rows, key_rows, value_rows, query_tangent, key_tangent, value_tangent, query_gain, key_gain):

    def unblock(blocked):
        return blocked.reshape(GROUP, IMAGES, ROWS, HEADS, HD).transpose(1, 0, 2, 3, 4).reshape(IMAGES, SEQ, HEADS, HD)
    cosine, sine = rotation(0, SEQ, HD)
    cosine = cosine[None, :, None, :]
    sine = sine[None, :, None, :]
    partner = rotation_partner(HD)
    query_hat, query_dot = normalize(unblock(query_rows), unblock(query_tangent), query_gain, cosine, sine, partner)
    key_hat, key_dot = normalize(unblock(key_rows), unblock(key_tangent), key_gain, cosine, sine, partner)

    def per_head_split(feature_field):
        return feature_field.transpose(0, 2, 1, 3).reshape(IMAGES * HEADS, SEQ, HD)
    items = tuple((per_head_split(feature_field) for feature_field in (query_hat, query_dot, key_hat, key_dot, unblock(value_rows), unblock(value_tangent))))
    attention_output, output_tangent = lax.map(attend, items)

    def regroup_blocks(feature_field):
        feature_field = feature_field.reshape(IMAGES, HEADS, SEQ, HD).transpose(0, 2, 1, 3)
        feature_field = feature_field.reshape(IMAGES, GROUP, ROWS, HEADS * HD).transpose(1, 0, 2, 3)
        return feature_field.reshape(GROUP * IMAGES, ROWS, HEADS * HD)
    return (regroup_blocks(attention_output), regroup_blocks(output_tangent))
```

```python
import math

import jax
import jax.numpy as jnp
from jax import lax
from jax.experimental import pallas as pl
from jax.experimental.pallas import tpu as pltpu
from jax.sharding import PartitionSpec as P

HD = 128
TXT = 512
GRID_W = 64
IMAGES = 4
RING = 8
PART = 18
BLOCK = RING * PART
STREAMS = 3
PIECES = 8
ITEMS = STREAMS * PIECES
LAG = 1

EPSILON = 1e-06
THETA = 10000.0
SCALE = 1.0 / math.sqrt(HD)
MESH = pl.DeviceIdType.MESH


def rows_at(slot):
    return pl.ds(pl.multiple_of(slot * BLOCK, 16), BLOCK)


def columns_at(head):
    return pl.ds(pl.multiple_of(head * HD, HD), HD)


def kernel(
    query_ref,
    key_ref,
    value_ref,
    query_tan_ref,
    key_tan_ref,
    value_tan_ref,
    query_gain_ref,
    key_gain_ref,
    out_ref,
    out_tan_ref,
    packed,
    landed,
    queries,
    store,
    peak,
    total,
    drift,
    summed,
    result,
    returned,
    kv_send,
    kv_recv,
    q_send,
    q_recv,
    ag_send,
    ag_recv,
    back_send,
    back_recv,
):
    head = lax.axis_index("head")
    blk = lax.axis_index("blk")
    core = head % 2
    x = blk % IMAGES
    y = (head // 2) * 2 + (blk // IMAGES) % 2
    z = blk // (2 * IMAGES)

    def device(yy, zz, cc):
        return {"head": (yy // 2) * 2 + cc, "blk": (zz * 2 + yy % 2) * IMAGES + x}

    def spread(stream, hops):
        flip = stream % 2
        return device((y + hops * (1 - flip)) % RING, (z + hops * flip) % RING, core)

    def along(stream, hops):
        flip = stream % 2
        return device((y + hops * flip) % RING, (z + hops * (1 - flip)) % RING, core)

    partner = device(y, z, 1 - core)

    def head_of(stream, hops):
        if stream == 1:
            return 2 * RING + (z + hops) % RING
        return 2 * ((y + hops) % RING) + stream // 2

    barrier = pltpu.get_barrier_semaphore()

    def greet(k, carry):
        pl.semaphore_signal(barrier, inc=1, device_id=spread(0, k), device_id_type=MESH)
        pl.semaphore_signal(barrier, inc=1, device_id=spread(1, k), device_id_type=MESH)
        return carry

    lax.fori_loop(1, RING, greet, 0)
    pl.semaphore_signal(barrier, inc=1, device_id=partner, device_id_type=MESH)

    place = blk // IMAGES
    token = place * BLOCK + head * PART + lax.broadcasted_iota(jnp.int32, (PART, HD), 0)
    lane = lax.broadcasted_iota(jnp.int32, (PART, HD), 1)
    pair = lax.shift_right_logical(lane, 1)
    patch = jnp.maximum(token - TXT, 0)
    row_id = lax.shift_right_logical(patch, 6).astype(jnp.float32)
    column_id = (patch & (GRID_W - 1)).astype(jnp.float32)
    in_row = pair < 36
    step = jnp.where(in_row, pair - 8, pair - 36).astype(jnp.float32)
    frequency = jnp.exp(-math.log(THETA) * (step * (2.0 / 56)))
    angle = jnp.where(in_row, row_id, column_id) * frequency
    angle = jnp.where(pair < 8, 0.0, angle)
    odd = (lane & 1) == 1
    cosine = jnp.cos(angle)
    sine = jnp.sin(angle)
    sine = jnp.where(odd, sine, -sine)

    def rotate(v):
        swapped = jnp.where(odd, pltpu.roll(v, 1, 1), pltpu.roll(v, HD - 1, 1))
        return v * cosine + swapped * sine

    def normalize(raw, tangent, gain):
        values = raw.astype(jnp.float32)
        motion = tangent.astype(jnp.float32)
        inverse = lax.rsqrt(jnp.mean(values * values, axis=-1, keepdims=True) + EPSILON)
        coupling = jnp.mean(values * motion, axis=-1, keepdims=True)
        normed = values * inverse * gain
        normed_dot = gain * (
            motion * inverse - values * (inverse * inverse * inverse * coupling)
        )
        return rotate(normed).astype(jnp.bfloat16), rotate(normed_dot).astype(jnp.bfloat16)

    query_gain = query_gain_ref[...]
    key_gain = key_gain_ref[...]

    def pack(k, carry):
        for stream in range(STREAMS):
            cols = columns_at(head_of(stream, k))
            query_hat, query_dot = normalize(
                query_ref[0, :, cols], query_tan_ref[0, :, cols], query_gain
            )
            key_hat, key_dot = normalize(
                key_ref[0, :, cols], key_tan_ref[0, :, cols], key_gain
            )
            arrays = (
                query_hat,
                query_dot,
                key_hat,
                key_dot,
                value_ref[0, :, cols],
                value_tan_ref[0, :, cols],
            )
            for a, v in enumerate(arrays):
                packed[k, stream, a, 0:8] = v[0:16].reshape(8, 2, HD)
                packed[k, stream, a, 8] = v[16:18]
        return carry

    lax.fori_loop(0, RING, pack, 0)
    for stream in range(STREAMS):
        landed[stream, :, 0:9] = packed[0, stream]

    pl.semaphore_wait(barrier, 2 * RING - 1)

    def kv_copy(stream, k):
        return pltpu.make_async_remote_copy(
            src_ref=packed.at[k, stream, pl.ds(2, 4)],
            dst_ref=landed.at[stream, pl.ds(2, 4), pl.ds(k * 9, 9)],
            send_sem=kv_send.at[stream, k],
            recv_sem=kv_recv.at[stream, k],
            device_id=spread(stream, k),
            device_id_type=MESH,
        )

    def q_copy(stream, k):
        return pltpu.make_async_remote_copy(
            src_ref=packed.at[k, stream, pl.ds(0, 2)],
            dst_ref=landed.at[stream, pl.ds(0, 2), pl.ds(k * 9, 9)],
            send_sem=q_send.at[stream, k],
            recv_sem=q_recv.at[stream, k],
            device_id=spread(stream, k),
            device_id_type=MESH,
        )

    def for_peers(action):
        def one(k, carry):
            action(k)
            return carry

        lax.fori_loop(1, RING, one, 0)

    for stream in range(STREAMS):
        for_peers(lambda k: kv_copy(stream, k).start())
    for stream in range(STREAMS):
        for_peers(lambda k: q_copy(stream, k).start())

    def ag_copy(stream, source, target, pair_of, to):
        return pltpu.make_async_remote_copy(
            src_ref=store.at[stream, pl.ds(2 * pair_of, 2), rows_at(source)],
            dst_ref=store.at[stream, pl.ds(2 * pair_of, 2), rows_at(target)],
            send_sem=ag_send.at[stream, target, pair_of],
            recv_sem=ag_recv.at[stream, target, pair_of],
            device_id=to,
            device_id_type=MESH,
        )

    def arrived(stream, slot, pair_of):
        ag_copy(stream, slot, slot, pair_of, partner).wait_recv()

    for stream in range(STREAMS):
        for_peers(lambda k: kv_copy(stream, k).wait_recv())
        for a in range(4):
            store[stream, a, 0:BLOCK] = landed.at[stream, 2 + a].reshape(BLOCK, HD)[...]
        for pair_of in range(2):
            ag_copy(stream, 0, 2, pair_of, along(stream, 1)).start()
            ag_copy(stream, 0, 4, pair_of, along(stream, RING - 1)).start()
        for pair_of in range(2):
            ag_copy(stream, 0, 1, pair_of, partner).start()

    for stream in range(STREAMS):
        for_peers(lambda k: q_copy(stream, k).wait_recv())
        query_hat = landed.at[stream, 0].reshape(BLOCK, HD)[...]
        query_dot = landed.at[stream, 1].reshape(BLOCK, HD)[...]
        queries[stream, :, 0:HD] = query_dot
        queries[stream, :, HD : 2 * HD] = query_hat
        peak[stream] = jnp.full((BLOCK, 1), -jnp.inf, jnp.float32)
        total[stream] = jnp.zeros((BLOCK, 1), jnp.float32)
        drift[stream] = jnp.zeros((BLOCK, 1), jnp.float32)
        summed[stream] = jnp.zeros((BLOCK, 2 * HD), jnp.float32)

    def pass_on(item):
        stream = item % STREAMS
        piece = item // STREAMS
        slot = 2 * piece
        onward = along(stream, 1 + (piece + 1) % 2 * (RING - 2))
        for pair_of in range(2):
            arrived(stream, slot, pair_of)

            @pl.when(piece <= 4)
            def _():
                ag_copy(stream, slot, slot + 4, pair_of, onward).start()

            @pl.when(piece == 5 + pair_of)
            def _():
                ag_copy(stream, slot, 14, pair_of, onward).start()

            ag_copy(stream, slot, slot + 1, pair_of, partner).start()

    def absorb(item):
        stream = item % STREAMS
        piece = item // STREAMS
        for pair_of in range(2):
            arrived(stream, 2 * piece + 1, pair_of)
        rows = pl.ds(pl.multiple_of(piece * (2 * BLOCK), 32), 2 * BLOCK)
        query_pair = queries[stream]
        query_hat = query_pair[:, HD:]
        key = store[stream, 0, rows]
        key_pair = jnp.concatenate([key, store[stream, 1, rows]], axis=1)
        value = store[stream, 2, rows]
        value_pair = jnp.concatenate([value, store[stream, 3, rows]], axis=1)
        contract = (((1,), (1,)), ((), ()))
        scores = (
            lax.dot_general(query_hat, key, contract, preferred_element_type=jnp.float32)
            * SCALE
        )
        scores_dot = (
            lax.dot_general(
                query_pair, key_pair, contract, preferred_element_type=jnp.float32
            )
            * SCALE
        )
        old_peak = peak[stream]
        new_peak = jnp.maximum(old_peak, jnp.max(scores, axis=1, keepdims=True))
        rescale = jnp.exp(old_peak - new_peak)
        weights = jnp.exp(scores - new_peak)
        product = weights * scores_dot
        peak[stream] = new_peak
        total[stream] = total[stream] * rescale + jnp.sum(weights, axis=1, keepdims=True)
        drift[stream] = drift[stream] * rescale + jnp.sum(product, axis=1, keepdims=True)
        low_weights = weights.astype(jnp.bfloat16)
        low_product = product.astype(jnp.bfloat16)
        first = jnp.dot(low_weights, value_pair, preferred_element_type=jnp.float32)
        second = jnp.dot(low_product, value, preferred_element_type=jnp.float32)
        summed[stream, :, 0:HD] = summed[stream, :, 0:HD] * rescale + first[:, 0:HD]
        summed[stream, :, HD:] = (
            summed[stream, :, HD:] * rescale + first[:, HD:] + second
        )

    def advance(item, carry):
        @pl.when((item >= STREAMS) & (item < ITEMS))
        def _():
            pass_on(item)

        absorb(item - LAG)
        return carry

    lax.fori_loop(LAG, ITEMS + LAG, advance, 0)

    def back_copy(stream, k):
        return pltpu.make_async_remote_copy(
            src_ref=result.at[stream, :, pl.ds(k * 9, 9)],
            dst_ref=returned.at[k, stream],
            send_sem=back_send.at[stream, k],
            recv_sem=back_recv.at[stream, k],
            device_id=spread(stream, RING - k),
            device_id_type=MESH,
        )

    for stream in range(STREAMS):
        inverse = 1.0 / total[stream]
        base = summed[stream, :, 0:HD]
        attended = base * inverse
        tangent = (summed[stream, :, HD:] - drift[stream] * inverse * base) * inverse
        result.at[stream, 0].reshape(BLOCK, HD)[...] = attended.astype(jnp.bfloat16)
        result.at[stream, 1].reshape(BLOCK, HD)[...] = tangent.astype(jnp.bfloat16)
        for_peers(lambda k: back_copy(stream, k).start())

    def unpack(stream, k):
        cols = columns_at(head_of(stream, k))
        for a, ref in enumerate((out_ref, out_tan_ref)):
            ref[0, 0:16, cols] = returned[k, stream, a, 0:8].reshape(16, HD)
            ref[0, 16:18, cols] = returned[k, stream, a, 8]

    for stream in range(STREAMS):
        returned[0, stream] = result[stream, :, 0:9]
        unpack(stream, 0)

    for stream in range(STREAMS):

        def finish(k):
            back_copy(stream, k).wait_recv()
            unpack(stream, k)

        for_peers(finish)

    for stream in range(STREAMS):

        def settle(k):
            kv_copy(stream, k).wait_send()
            q_copy(stream, k).wait_send()
            back_copy(stream, k).wait_send()

        for_peers(settle)

        def settle_ring(slot, carry):
            for pair_of in range(2):
                ag_copy(stream, slot, slot, pair_of, partner).wait_send()
            return carry

        lax.fori_loop(1, 2 * PIECES, settle_ring, 0)


def local(*operands):
    arrays, gains = operands[:6], operands[6:]
    shape = jax.ShapeDtypeStruct((1, PART, arrays[0].shape[2]), jnp.bfloat16)
    vmem = pl.BlockSpec(memory_space=pltpu.VMEM)
    dma = pltpu.SemaphoreType.DMA
    bf16, f32 = jnp.bfloat16, jnp.float32
    out = pl.pallas_call(
        kernel,
        out_shape=(shape, shape),
        in_specs=[vmem] * 8,
        out_specs=(vmem, vmem),
        scratch_shapes=[
            pltpu.VMEM((RING, STREAMS, 6, 9, 2, HD), bf16),
            pltpu.VMEM((STREAMS, 6, 72, 2, HD), bf16),
            pltpu.VMEM((STREAMS, BLOCK, 2 * HD), bf16),
            pltpu.VMEM((STREAMS, 4, 2 * PIECES * BLOCK, HD), bf16),
            pltpu.VMEM((STREAMS, BLOCK, 1), f32),
            pltpu.VMEM((STREAMS, BLOCK, 1), f32),
            pltpu.VMEM((STREAMS, BLOCK, 1), f32),
            pltpu.VMEM((STREAMS, BLOCK, 2 * HD), f32),
            pltpu.VMEM((STREAMS, 2, 72, 2, HD), bf16),
            pltpu.VMEM((RING, STREAMS, 2, 9, 2, HD), bf16),
            dma((STREAMS, RING)),
            dma((STREAMS, RING)),
            dma((STREAMS, RING)),
            dma((STREAMS, RING)),
            dma((STREAMS, 2 * PIECES, 2)),
            dma((STREAMS, 2 * PIECES, 2)),
            dma((STREAMS, RING)),
            dma((STREAMS, RING)),
        ],
        compiler_params=pltpu.CompilerParams(
            collective_id=0,
            has_side_effects=True,
            vmem_limit_bytes=40 * 1024 * 1024,
        ),
    )(*arrays, *(g.reshape(1, HD) for g in gains))
    return out[0], out[1]


def solution(mesh):
    rows = P("blk", "head", None)
    return jax.shard_map(
        local,
        mesh=mesh,
        in_specs=(rows,) * 6 + (P(), P()),
        out_specs=(rows, rows),
        check_vma=False,
    )
```

```python
import math

import jax
import jax.numpy as jnp
from jax import lax
from jax.experimental import pallas as pl
from jax.experimental.pallas import tpu as pltpu
from jax.sharding import PartitionSpec as P

HD = 128
TXT = 512
GRID_W = 64
IMAGES = 4
RING = 8
PART = 18
BLOCK = RING * PART
STREAMS = 3
PIECES = 8
PASS, ABSORB = 0, 1
ORDER = (
    (PASS, 1, 0, 1), (PASS, 0, 0, 1), (PASS, 1, 0, 0), (PASS, 0, 0, 0), (ABSORB, 1, 0, 1),
    (PASS, 0, 1, 1), (PASS, 0, 2, 1), (PASS, 2, 0, 1), (PASS, 0, 1, 0), (PASS, 0, 2, 0),
    (PASS, 2, 0, 0), (PASS, 0, 3, 1), (PASS, 0, 4, 1), (ABSORB, 0, 0, 1), (PASS, 2, 1, 1),
    (PASS, 2, 2, 1), (ABSORB, 0, 1, 2), (ABSORB, 2, 0, 1), (PASS, 0, 3, 0), (PASS, 0, 4, 0),
    (PASS, 1, 1, 1), (PASS, 1, 2, 1), (PASS, 2, 1, 0), (PASS, 2, 2, 0), (PASS, 1, 1, 0),
    (PASS, 1, 2, 0), (ABSORB, 0, 3, 2), (PASS, 0, 5, 1), (PASS, 0, 6, 1), (ABSORB, 2, 1, 2),
    (PASS, 1, 3, 1), (PASS, 1, 4, 1), (PASS, 2, 3, 1), (PASS, 2, 4, 1), (ABSORB, 1, 1, 2),
    (PASS, 1, 3, 0), (PASS, 1, 4, 0), (PASS, 0, 5, 0), (PASS, 0, 6, 0), (PASS, 2, 3, 0),
    (PASS, 2, 4, 0), (PASS, 1, 5, 1), (PASS, 1, 6, 1), (ABSORB, 1, 3, 2), (PASS, 2, 5, 1),
    (PASS, 0, 7, 1), (PASS, 1, 5, 0), (PASS, 1, 6, 0), (ABSORB, 0, 5, 2), (PASS, 0, 7, 0),
    (PASS, 2, 6, 1), (ABSORB, 2, 3, 2), (PASS, 1, 7, 1), (PASS, 2, 5, 0), (PASS, 2, 6, 0),
    (ABSORB, 1, 5, 2), (PASS, 1, 7, 0), (ABSORB, 0, 7, 1), (PASS, 2, 7, 1), (ABSORB, 2, 5, 2),
    (ABSORB, 1, 7, 1), (PASS, 2, 7, 0), (ABSORB, 2, 7, 1),
)
QUERY, KEY, VALUE = 0, 1, 2

EPSILON = 1e-06
THETA = 10000.0
SCALE = 1.0 / math.sqrt(HD)
MESH = pl.DeviceIdType.MESH


def rows_at(slot):
    return pl.ds(slot * BLOCK, BLOCK)


def columns_at(head):
    return pl.ds(pl.multiple_of(head * HD, HD), HD)


def kernel(
    query_hbm,
    key_hbm,
    value_hbm,
    query_tan_hbm,
    key_tan_hbm,
    value_tan_hbm,
    query_gain_hbm,
    key_gain_hbm,
    out_ref,
    out_tan_ref,
    inputs,
    gains,
    packed,
    landed,
    queries,
    store,
    peak,
    total,
    drift,
    summed,
    result,
    returned,
    input_sem,
    spread_send,
    spread_recv,
    ring_send,
    ring_recv,
    partner_recv,
    back_send,
    back_recv,
):
    sources = (query_hbm, query_tan_hbm, key_hbm, key_tan_hbm, value_hbm, value_tan_hbm)
    loads = [
        pltpu.make_async_copy(source.at[0], inputs.at[a], input_sem.at[a])
        for a, source in enumerate(sources)
    ]
    for i, source in enumerate((query_gain_hbm, key_gain_hbm)):
        loads.append(pltpu.make_async_copy(source, gains.at[i], input_sem.at[6 + i]))
    for a in (4, 5, 2, 3, 7, 0, 1, 6):
        loads[a].start()

    head = lax.axis_index("head")
    blk = lax.axis_index("blk")
    core = head % 2
    x = blk % IMAGES
    y = (head // 2) * 2 + (blk // IMAGES) % 2
    z = blk // (2 * IMAGES)

    def device(yy, zz, cc):
        return {"head": (yy // 2) * 2 + cc, "blk": (zz * 2 + yy % 2) * IMAGES + x}

    def spread(stream, hops):
        flip = stream % 2
        return device((y + hops * (1 - flip)) % RING, (z + hops * flip) % RING, core)

    def along(stream, hops):
        flip = stream % 2
        return device((y + hops * flip) % RING, (z + hops * (1 - flip)) % RING, core)

    partner = device(y, z, 1 - core)

    def head_of(stream, hops):
        if stream == 1:
            return 2 * RING + (z + hops) % RING
        return 2 * ((y + hops) % RING) + stream // 2

    barrier = pltpu.get_barrier_semaphore()

    def greet(k, carry):
        pl.semaphore_signal(barrier, inc=1, device_id=spread(0, k), device_id_type=MESH)
        pl.semaphore_signal(barrier, inc=1, device_id=spread(1, k), device_id_type=MESH)
        return carry

    lax.fori_loop(1, RING, greet, 0)
    pl.semaphore_signal(barrier, inc=1, device_id=partner, device_id_type=MESH)

    place = blk // IMAGES
    token = place * BLOCK + head * PART + lax.broadcasted_iota(jnp.int32, (PART, HD), 0)
    lane = lax.broadcasted_iota(jnp.int32, (PART, HD), 1)
    pair = lax.shift_right_logical(lane, 1)
    patch = jnp.maximum(token - TXT, 0)
    row_id = lax.shift_right_logical(patch, 6).astype(jnp.float32)
    column_id = (patch & (GRID_W - 1)).astype(jnp.float32)
    in_row = pair < 36
    step = jnp.where(in_row, pair - 8, pair - 36).astype(jnp.float32)
    frequency = jnp.exp(-math.log(THETA) * (step * (2.0 / 56)))
    angle = jnp.where(in_row, row_id, column_id) * frequency
    angle = jnp.where(pair < 8, 0.0, angle)
    odd = (lane & 1) == 1
    cosine = jnp.cos(angle)
    sine = jnp.sin(angle)
    sine = jnp.where(odd, sine, -sine)

    def rotate(v):
        swapped = jnp.where(odd, pltpu.roll(v, 1, 1), pltpu.roll(v, HD - 1, 1))
        return v * cosine + swapped * sine

    def normalize(raw, tangent, gain):
        values = raw.astype(jnp.float32)
        motion = tangent.astype(jnp.float32)
        inverse = lax.rsqrt(jnp.mean(values * values, axis=-1, keepdims=True) + EPSILON)
        coupling = jnp.mean(values * motion, axis=-1, keepdims=True)
        normed = values * inverse * gain
        normed_dot = gain * (
            motion * inverse - values * (inverse * inverse * inverse * coupling)
        )
        return rotate(normed).astype(jnp.bfloat16), rotate(normed_dot).astype(jnp.bfloat16)

    def put(k, stream, a, v):
        packed[k, stream, a, 0:8] = v[0:16].reshape(8, 2, HD)
        packed[k, stream, a, 8] = v[16:18]

    def pack(stream, group):
        def one(k, carry):
            cols = columns_at(head_of(stream, k))
            raw, tangent = inputs[2 * group, :, cols], inputs[2 * group + 1, :, cols]
            if group != VALUE:
                raw, tangent = normalize(raw, tangent, gains[group])
            put(k, stream, 2 * group, raw)
            put(k, stream, 2 * group + 1, tangent)
            return carry

        lax.fori_loop(0, RING, one, 0, unroll=4)
        pair = pl.ds(2 * group, 2)
        landed[stream, pair, 0:9] = packed[0, stream, pair]

    def spread_copy(stream, group, k):
        pair = pl.ds(2 * group, 2)
        return pltpu.make_async_remote_copy(
            src_ref=packed.at[k, stream, pair],
            dst_ref=landed.at[stream, pair, pl.ds(k * 9, 9)],
            send_sem=spread_send,
            recv_sem=spread_recv.at[stream, group],
            device_id=spread(stream, k),
            device_id_type=MESH,
        )

    def send_out(stream, group):
        def one(k, carry):
            spread_copy(stream, group, k).start()
            return carry

        lax.fori_loop(1, RING, one, 0)

    def await_bytes(ref, sem):
        pltpu.make_async_copy(ref, ref, sem).wait()

    for a in (4, 5):
        loads[a].wait()
    for stream in range(STREAMS):
        pack(stream, VALUE)
    for a in (2, 3, 7):
        loads[a].wait()
    for stream in (0, 1):
        pack(stream, KEY)
    pl.semaphore_wait(barrier, 2 * RING - 1)
    for group in (VALUE, KEY):
        for stream in (0, 1):
            send_out(stream, group)
    send_out(2, VALUE)
    pack(2, KEY)
    send_out(2, KEY)
    for a in (0, 1, 6):
        loads[a].wait()
    for stream in (1, 0, 2):
        pack(stream, QUERY)
        send_out(stream, QUERY)

    def ring_copy(stream, source, target, pair_of, to):
        pair = pl.ds(2 * pair_of, 2)
        return pltpu.make_async_remote_copy(
            src_ref=store.at[stream, pair, rows_at(source)],
            dst_ref=store.at[stream, pair, rows_at(target)],
            send_sem=ring_send.at[stream],
            recv_sem=ring_recv.at[stream, target // 2, pair_of],
            device_id=to,
            device_id_type=MESH,
        )

    def hand_over(stream, source, pair_of):
        pair = pl.ds(2 * pair_of, 2)
        return pltpu.make_async_remote_copy(
            src_ref=store.at[stream, pair, rows_at(source)],
            dst_ref=store.at[stream, pair, rows_at(source + 1)],
            send_sem=ring_send.at[stream],
            recv_sem=partner_recv.at[stream, source // 2],
            device_id=partner,
            device_id_type=MESH,
        )

    def begin(stream, pair_of):
        pair = pl.ds(2 * (pair_of + 1), 2)
        await_bytes(
            landed.at[stream, pair, pl.ds(9, 63)], spread_recv.at[stream, pair_of + 1]
        )
        for a in (2 * pair_of, 2 * pair_of + 1):
            store[stream, a, 0:BLOCK] = landed.at[stream, 2 + a].reshape(BLOCK, HD)[...]
        ring_copy(stream, 0, 2, pair_of, along(stream, 1)).start()
        ring_copy(stream, 0, 4, pair_of, along(stream, RING - 1)).start()
        hand_over(stream, 0, pair_of).start()

    def pass_on(stream, piece, pair_of):
        slot = 2 * piece
        await_bytes(
            store.at[stream, pl.ds(2 * pair_of, 2), rows_at(slot)],
            ring_recv.at[stream, piece, pair_of],
        )
        onward = along(stream, 1 if piece % 2 else RING - 1)
        if piece <= 4:
            ring_copy(stream, slot, slot + 4, pair_of, onward).start()
        elif piece == 5 + pair_of:
            ring_copy(stream, slot, 14, pair_of, onward).start()
        hand_over(stream, slot, pair_of).start()

    def open_queries(stream):
        await_bytes(
            landed.at[stream, pl.ds(0, 2), pl.ds(9, 63)], spread_recv.at[stream, QUERY]
        )
        query_hat = landed.at[stream, 0].reshape(BLOCK, HD)[...]
        query_dot = landed.at[stream, 1].reshape(BLOCK, HD)[...]
        queries[stream, :, 0:HD] = query_dot
        queries[stream, :, HD : 2 * HD] = query_hat
        peak[stream] = jnp.full((BLOCK, 1), -jnp.inf, jnp.float32)
        total[stream] = jnp.zeros((BLOCK, 1), jnp.float32)
        drift[stream] = jnp.zeros((BLOCK, 1), jnp.float32)
        summed[stream] = jnp.zeros((BLOCK, 2 * HD), jnp.float32)

    def absorb(stream, first_piece, count):
        for piece in range(first_piece, first_piece + count):
            await_bytes(
                store.at[stream, :, rows_at(2 * piece + 1)],
                partner_recv.at[stream, piece],
            )
        rows = pl.ds(first_piece * (2 * BLOCK), count * (2 * BLOCK))
        query_pair = queries[stream]
        query_hat = query_pair[:, HD:]
        key = store[stream, 0, rows]
        key_pair = jnp.concatenate([key, store[stream, 1, rows]], axis=1)
        value = store[stream, 2, rows]
        value_pair = jnp.concatenate([value, store[stream, 3, rows]], axis=1)
        contract = (((1,), (1,)), ((), ()))
        scores = (
            lax.dot_general(query_hat, key, contract, preferred_element_type=jnp.float32)
            * SCALE
        )
        scores_dot = (
            lax.dot_general(
                query_pair, key_pair, contract, preferred_element_type=jnp.float32
            )
            * SCALE
        )
        old_peak = peak[stream]
        new_peak = jnp.maximum(old_peak, jnp.max(scores, axis=1, keepdims=True))
        rescale = jnp.exp(old_peak - new_peak)
        weights = jnp.exp(scores - new_peak)
        product = weights * scores_dot
        peak[stream] = new_peak
        total[stream] = total[stream] * rescale + jnp.sum(weights, axis=1, keepdims=True)
        drift[stream] = drift[stream] * rescale + jnp.sum(product, axis=1, keepdims=True)
        low_weights = weights.astype(jnp.bfloat16)
        low_product = product.astype(jnp.bfloat16)
        first = jnp.dot(low_weights, value_pair, preferred_element_type=jnp.float32)
        second = jnp.dot(low_product, value, preferred_element_type=jnp.float32)
        summed[stream, :, 0:HD] = summed[stream, :, 0:HD] * rescale + first[:, 0:HD]
        summed[stream, :, HD:] = (
            summed[stream, :, HD:] * rescale + first[:, HD:] + second
        )

    def back_copy(stream, k):
        return pltpu.make_async_remote_copy(
            src_ref=result.at[stream, :, pl.ds(k * 9, 9)],
            dst_ref=returned.at[k, stream],
            send_sem=back_send,
            recv_sem=back_recv.at[stream],
            device_id=spread(stream, RING - k),
            device_id_type=MESH,
        )

    def finish(stream):
        inverse = 1.0 / total[stream]
        base = summed[stream, :, 0:HD]
        attended = base * inverse
        tangent = (summed[stream, :, HD:] - drift[stream] * inverse * base) * inverse
        result.at[stream, 0].reshape(BLOCK, HD)[...] = attended.astype(jnp.bfloat16)
        result.at[stream, 1].reshape(BLOCK, HD)[...] = tangent.astype(jnp.bfloat16)

        def one(k, carry):
            back_copy(stream, k).start()
            return carry

        lax.fori_loop(1, RING, one, 0)
        returned[0, stream] = result[stream, :, 0:9]

    for kind, stream, piece, detail in ORDER:
        if kind == PASS and piece == 0:
            begin(stream, detail)
        elif kind == PASS:
            pass_on(stream, piece, detail)
        else:
            if piece == 0:
                open_queries(stream)
            absorb(stream, piece, detail)
            if piece == PIECES - 1:
                finish(stream)

    for stream in range(STREAMS):
        await_bytes(returned.at[pl.ds(1, 7), stream], back_recv.at[stream])

        def unpack(k, carry):
            cols = columns_at(head_of(stream, k))
            for a, ref in enumerate((out_ref, out_tan_ref)):
                ref[0, 0:16, cols] = returned[k, stream, a, 0:8].reshape(16, HD)
                ref[0, 16:18, cols] = returned[k, stream, a, 8]
            return carry

        lax.fori_loop(0, RING, unpack, 0, unroll=4)

    await_bytes(packed.at[pl.ds(1, 7)], spread_send)
    await_bytes(result.at[:, :, pl.ds(9, 63)], back_send)
    for stream in range(STREAMS):
        await_bytes(
            store.at[stream, :, pl.ds(BLOCK, (2 * PIECES - 1) * BLOCK)],
            ring_send.at[stream],
        )


def local(*operands):
    operands = operands[:6] + tuple(g.reshape(1, HD) for g in operands[6:])
    shape = jax.ShapeDtypeStruct(operands[0].shape, jnp.bfloat16)
    vmem = pl.BlockSpec(memory_space=pltpu.VMEM)
    dma = pltpu.SemaphoreType.DMA
    bf16, f32 = jnp.bfloat16, jnp.float32
    out = pl.pallas_call(
        kernel,
        out_shape=(shape, shape),
        in_specs=[pl.BlockSpec(memory_space=pltpu.HBM)] * 8,
        out_specs=(vmem, vmem),
        scratch_shapes=[
            pltpu.VMEM((6, PART, operands[0].shape[2]), bf16),
            pltpu.VMEM((2, 1, HD), f32),
            pltpu.VMEM((RING, STREAMS, 6, 9, 2, HD), bf16),
            pltpu.VMEM((STREAMS, 6, 72, 2, HD), bf16),
            pltpu.VMEM((STREAMS, BLOCK, 2 * HD), bf16),
            pltpu.VMEM((STREAMS, 4, 2 * PIECES * BLOCK, HD), bf16),
            pltpu.VMEM((STREAMS, BLOCK, 1), f32),
            pltpu.VMEM((STREAMS, BLOCK, 1), f32),
            pltpu.VMEM((STREAMS, BLOCK, 1), f32),
            pltpu.VMEM((STREAMS, BLOCK, 2 * HD), f32),
            pltpu.VMEM((STREAMS, 2, 72, 2, HD), bf16),
            pltpu.VMEM((RING, STREAMS, 2, 9, 2, HD), bf16),
            dma((8,)),
            dma,
            dma((STREAMS, 3)),
            dma((STREAMS,)),
            dma((STREAMS, PIECES, 2)),
            dma((STREAMS, PIECES)),
            dma,
            dma((STREAMS,)),
        ],
        compiler_params=pltpu.CompilerParams(
            collective_id=0,
            has_side_effects=True,
            vmem_limit_bytes=40 * 1024 * 1024,
        ),
    )(*(pltpu.with_memory_space_constraint(a, pltpu.HBM) for a in operands))
    return out[0], out[1]


def solution(mesh):
    rows = P("blk", "head", None)
    return jax.shard_map(
        local,
        mesh=mesh,
        in_specs=(rows,) * 6 + (P(), P()),
        out_specs=(rows, rows),
        check_vma=False,
    )
```

```python
import math

import jax
import jax.numpy as jnp
from jax import lax
from jax.experimental import pallas as pl
from jax.experimental.pallas import tpu as pltpu
from jax.sharding import PartitionSpec as P

HD = 128
TXT = 512
GRID_W = 64
IMAGES = 4
RING = 8
PART = 18
BLOCK = RING * PART
STREAMS = 3
PIECES = 8
PASS, ABSORB = 0, 1
ORDER = (
    (PASS, 1, 0, 1), (PASS, 0, 0, 1), (PASS, 0, 0, 0), (PASS, 1, 0, 0), (PASS, 0, 2, 1),
    (PASS, 0, 1, 1), (PASS, 2, 0, 1), (PASS, 2, 0, 0), (PASS, 0, 1, 0), (PASS, 0, 2, 0),
    (PASS, 2, 1, 1), (PASS, 2, 2, 1), (PASS, 1, 2, 1), (ABSORB, 0, 0, 1), (PASS, 2, 2, 0),
    (PASS, 2, 1, 0), (PASS, 1, 1, 0), (PASS, 0, 3, 1), (PASS, 1, 1, 1), (PASS, 1, 2, 0),
    (PASS, 0, 3, 0), (ABSORB, 1, 0, 1), (PASS, 0, 4, 0), (PASS, 0, 4, 1), (PASS, 2, 4, 1),
    (PASS, 1, 4, 1), (ABSORB, 2, 0, 1), (ABSORB, 2, 1, 2), (PASS, 1, 3, 0), (ABSORB, 0, 3, 2),
    (PASS, 2, 3, 0), (PASS, 2, 3, 1), (PASS, 1, 4, 0), (PASS, 2, 4, 0), (ABSORB, 0, 1, 2),
    (PASS, 1, 3, 1), (PASS, 1, 6, 1), (ABSORB, 2, 3, 2), (PASS, 0, 6, 0), (PASS, 0, 5, 1),
    (PASS, 1, 5, 0), (PASS, 0, 5, 0), (PASS, 0, 6, 1), (ABSORB, 1, 1, 2), (PASS, 1, 6, 0),
    (ABSORB, 1, 3, 2), (PASS, 2, 6, 1), (PASS, 1, 5, 1), (PASS, 2, 5, 0), (ABSORB, 0, 5, 2),
    (PASS, 1, 7, 1), (PASS, 2, 6, 0), (PASS, 2, 5, 1), (ABSORB, 1, 5, 2), (PASS, 1, 7, 0),
    (ABSORB, 2, 5, 2), (PASS, 0, 7, 0), (PASS, 0, 7, 1), (ABSORB, 1, 7, 1), (PASS, 2, 7, 1),
    (PASS, 2, 7, 0), (ABSORB, 0, 7, 1), (ABSORB, 2, 7, 1),
)
TURN = (1, 0, 0)
QUERY, KEY, VALUE = 0, 1, 2

EPSILON = 1e-06
THETA = 10000.0
SCALE = 1.0 / math.sqrt(HD)
MESH = pl.DeviceIdType.MESH


def rows_at(slot):
    return pl.ds(slot * BLOCK, BLOCK)


def columns_at(head):
    return pl.ds(pl.multiple_of(head * HD, HD), HD)


def kernel(
    query_hbm,
    key_hbm,
    value_hbm,
    query_tan_hbm,
    key_tan_hbm,
    value_tan_hbm,
    query_gain_hbm,
    key_gain_hbm,
    out_ref,
    out_tan_ref,
    inputs,
    gains,
    packed,
    landed,
    queries,
    store,
    peak,
    total,
    drift,
    summed,
    result,
    returned,
    input_sem,
    spread_send,
    spread_recv,
    ring_send,
    ring_recv,
    partner_recv,
    back_send,
    back_recv,
):
    head = lax.axis_index("head")
    blk = lax.axis_index("blk")
    core = head % 2
    x = blk % IMAGES
    y = (head // 2) * 2 + (blk // IMAGES) % 2
    z = blk // (2 * IMAGES)

    def device(yy, zz, cc):
        return {"head": (yy // 2) * 2 + cc, "blk": (zz * 2 + yy % 2) * IMAGES + x}

    def spread(stream, hops):
        flip = stream % 2
        return device((y + hops * (1 - flip)) % RING, (z + hops * flip) % RING, core)

    def along(stream, hops):
        flip = stream % 2
        return device((y + hops * flip) % RING, (z + hops * (1 - flip)) % RING, core)

    partner = device(y, z, 1 - core)

    def head_of(stream, hops):
        if stream == 1:
            return 2 * RING + (z + hops) % RING
        return 2 * ((y + hops) % RING) + stream // 2

    barrier = pltpu.get_barrier_semaphore()

    def peer(i):
        return RING // 2 + (i + 1) // 2 * (1 - 2 * (i % 2))

    def greet(i, carry):
        k = peer(i)
        pl.semaphore_signal(barrier, inc=1, device_id=spread(0, k), device_id_type=MESH)
        pl.semaphore_signal(barrier, inc=1, device_id=spread(1, k), device_id_type=MESH)
        return carry

    lax.fori_loop(0, RING - 1, greet, 0)
    pl.semaphore_signal(barrier, inc=1, device_id=partner, device_id_type=MESH)

    sources = (query_hbm, query_tan_hbm, key_hbm, key_tan_hbm, value_hbm, value_tan_hbm)
    loads = [
        pltpu.make_async_copy(source.at[0], inputs.at[a], input_sem.at[a])
        for a, source in enumerate(sources)
    ]
    for i, source in enumerate((query_gain_hbm, key_gain_hbm)):
        loads.append(pltpu.make_async_copy(source, gains.at[i], input_sem.at[6 + i]))
    for a in (4, 5, 2, 3, 7, 0, 1, 6):
        loads[a].start()

    place = blk // IMAGES
    token = place * BLOCK + head * PART + lax.broadcasted_iota(jnp.int32, (PART, HD), 0)
    lane = lax.broadcasted_iota(jnp.int32, (PART, HD), 1)
    pair = lax.shift_right_logical(lane, 1)
    patch = jnp.maximum(token - TXT, 0)
    row_id = lax.shift_right_logical(patch, 6).astype(jnp.float32)
    column_id = (patch & (GRID_W - 1)).astype(jnp.float32)
    in_row = pair < 36
    step = jnp.where(in_row, pair - 8, pair - 36).astype(jnp.float32)
    frequency = jnp.exp(-math.log(THETA) * (step * (2.0 / 56)))
    angle = jnp.where(in_row, row_id, column_id) * frequency
    angle = jnp.where(pair < 8, 0.0, angle)
    odd = (lane & 1) == 1
    cosine = jnp.cos(angle)
    sine = jnp.sin(angle)
    sine = jnp.where(odd, sine, -sine)

    def rotate(v):
        swapped = jnp.where(odd, pltpu.roll(v, 1, 1), pltpu.roll(v, HD - 1, 1))
        return v * cosine + swapped * sine

    def normalize(raw, tangent, gain):
        values = raw.astype(jnp.float32)
        motion = tangent.astype(jnp.float32)
        inverse = lax.rsqrt(jnp.mean(values * values, axis=-1, keepdims=True) + EPSILON)
        coupling = jnp.mean(values * motion, axis=-1, keepdims=True)
        normed = values * inverse * gain
        normed_dot = gain * (
            motion * inverse - values * (inverse * inverse * inverse * coupling)
        )
        return rotate(normed).astype(jnp.bfloat16), rotate(normed_dot).astype(jnp.bfloat16)

    def put(k, stream, a, v):
        packed[k, stream, a, 0:8] = v[0:16].reshape(8, 2, HD)
        packed[k, stream, a, 8] = v[16:18]

    def pack(stream, group):
        def one(k, carry):
            cols = columns_at(head_of(stream, k))
            raw, tangent = inputs[2 * group, :, cols], inputs[2 * group + 1, :, cols]
            if group != VALUE:
                raw, tangent = normalize(raw, tangent, gains[group])
            put(k, stream, 2 * group, raw)
            put(k, stream, 2 * group + 1, tangent)
            return carry

        lax.fori_loop(0, RING, one, 0, unroll=4)
        pair = pl.ds(2 * group, 2)
        landed[stream, pair, 0:9] = packed[0, stream, pair]

    def spread_copy(stream, group, k):
        pair = pl.ds(2 * group, 2)
        return pltpu.make_async_remote_copy(
            src_ref=packed.at[k, stream, pair],
            dst_ref=landed.at[stream, pair, pl.ds(k * 9, 9)],
            send_sem=spread_send,
            recv_sem=spread_recv.at[stream, group],
            device_id=spread(stream, k),
            device_id_type=MESH,
        )

    def send_out(stream, group):
        def one(i, carry):
            spread_copy(stream, group, peer(i)).start()
            return carry

        lax.fori_loop(0, RING - 1, one, 0)

    def await_bytes(ref, sem):
        pltpu.make_async_copy(ref, ref, sem).wait()

    for a in (4, 5):
        loads[a].wait()
    for stream in range(STREAMS):
        pack(stream, VALUE)
    for a in (2, 3, 7):
        loads[a].wait()
    for stream in (0, 1):
        pack(stream, KEY)
    pl.semaphore_wait(barrier, 2 * RING - 1)
    for group in (VALUE, KEY):
        for stream in (0, 1):
            send_out(stream, group)
    send_out(2, VALUE)
    pack(2, KEY)
    send_out(2, KEY)
    for a in (0, 1, 6):
        loads[a].wait()
    for stream in (1, 0, 2):
        pack(stream, QUERY)
        send_out(stream, QUERY)

    def ring_copy(stream, source, target, pair_of, to):
        pair = pl.ds(2 * pair_of, 2)
        return pltpu.make_async_remote_copy(
            src_ref=store.at[stream, pair, rows_at(source)],
            dst_ref=store.at[stream, pair, rows_at(target)],
            send_sem=ring_send.at[stream],
            recv_sem=ring_recv.at[stream, target // 2, pair_of],
            device_id=to,
            device_id_type=MESH,
        )

    def hand_over(stream, source, pair_of):
        pair = pl.ds(2 * pair_of, 2)
        return pltpu.make_async_remote_copy(
            src_ref=store.at[stream, pair, rows_at(source)],
            dst_ref=store.at[stream, pair, rows_at(source + 1)],
            send_sem=ring_send.at[stream],
            recv_sem=partner_recv.at[stream, source // 2],
            device_id=partner,
            device_id_type=MESH,
        )

    def begin(stream, pair_of):
        pair = pl.ds(2 * (pair_of + 1), 2)
        await_bytes(
            landed.at[stream, pair, pl.ds(9, 63)], spread_recv.at[stream, pair_of + 1]
        )
        for a in (2 * pair_of, 2 * pair_of + 1):
            store[stream, a, 0:BLOCK] = landed.at[stream, 2 + a].reshape(BLOCK, HD)[...]
        ring_copy(stream, 0, 2, pair_of, along(stream, 1)).start()
        ring_copy(stream, 0, 4, pair_of, along(stream, RING - 1)).start()
        hand_over(stream, 0, pair_of).start()

    def pass_on(stream, piece, pair_of):
        slot = 2 * piece
        await_bytes(
            store.at[stream, pl.ds(2 * pair_of, 2), rows_at(slot)],
            ring_recv.at[stream, piece, pair_of],
        )
        onward = along(stream, 1 if piece % 2 else RING - 1)
        if piece <= 4:
            ring_copy(stream, slot, slot + 4, pair_of, onward).start()
        elif piece == 5 + (pair_of ^ TURN[stream]):
            ring_copy(stream, slot, 14, pair_of, onward).start()
        hand_over(stream, slot, pair_of).start()

    def open_queries(stream):
        await_bytes(
            landed.at[stream, pl.ds(0, 2), pl.ds(9, 63)], spread_recv.at[stream, QUERY]
        )
        query_hat = landed.at[stream, 0].reshape(BLOCK, HD)[...]
        query_dot = landed.at[stream, 1].reshape(BLOCK, HD)[...]
        queries[stream, :, 0:HD] = query_dot
        queries[stream, :, HD : 2 * HD] = query_hat
        peak[stream] = jnp.full((BLOCK, 1), -jnp.inf, jnp.float32)
        total[stream] = jnp.zeros((BLOCK, 1), jnp.float32)
        drift[stream] = jnp.zeros((BLOCK, 1), jnp.float32)
        summed[stream] = jnp.zeros((BLOCK, 2 * HD), jnp.float32)

    def absorb(stream, first_piece, count):
        for piece in range(first_piece, first_piece + count):
            await_bytes(
                store.at[stream, :, rows_at(2 * piece + 1)],
                partner_recv.at[stream, piece],
            )
        rows = pl.ds(first_piece * (2 * BLOCK), count * (2 * BLOCK))
        query_pair = queries[stream]
        query_hat = query_pair[:, HD:]
        key = store[stream, 0, rows]
        key_pair = jnp.concatenate([key, store[stream, 1, rows]], axis=1)
        value = store[stream, 2, rows]
        value_pair = jnp.concatenate([value, store[stream, 3, rows]], axis=1)
        contract = (((1,), (1,)), ((), ()))
        scores = (
            lax.dot_general(query_hat, key, contract, preferred_element_type=jnp.float32)
            * SCALE
        )
        scores_dot = (
            lax.dot_general(
                query_pair, key_pair, contract, preferred_element_type=jnp.float32
            )
            * SCALE
        )
        old_peak = peak[stream]
        new_peak = jnp.maximum(old_peak, jnp.max(scores, axis=1, keepdims=True))
        rescale = jnp.exp(old_peak - new_peak)
        weights = jnp.exp(scores - new_peak)
        product = weights * scores_dot
        peak[stream] = new_peak
        total[stream] = total[stream] * rescale + jnp.sum(weights, axis=1, keepdims=True)
        drift[stream] = drift[stream] * rescale + jnp.sum(product, axis=1, keepdims=True)
        low_weights = weights.astype(jnp.bfloat16)
        low_product = product.astype(jnp.bfloat16)
        first = jnp.dot(low_weights, value_pair, preferred_element_type=jnp.float32)
        second = jnp.dot(low_product, value, preferred_element_type=jnp.float32)
        summed[stream, :, 0:HD] = summed[stream, :, 0:HD] * rescale + first[:, 0:HD]
        summed[stream, :, HD:] = (
            summed[stream, :, HD:] * rescale + first[:, HD:] + second
        )

    def back_copy(stream, k):
        return pltpu.make_async_remote_copy(
            src_ref=result.at[stream, :, pl.ds(k * 9, 9)],
            dst_ref=returned.at[k, stream],
            send_sem=back_send,
            recv_sem=back_recv.at[stream],
            device_id=spread(stream, RING - k),
            device_id_type=MESH,
        )

    def finish(stream):
        inverse = 1.0 / total[stream]
        base = summed[stream, :, 0:HD]
        attended = base * inverse
        tangent = (summed[stream, :, HD:] - drift[stream] * inverse * base) * inverse
        result.at[stream, 0].reshape(BLOCK, HD)[...] = attended.astype(jnp.bfloat16)
        result.at[stream, 1].reshape(BLOCK, HD)[...] = tangent.astype(jnp.bfloat16)

        def one(i, carry):
            back_copy(stream, peer(i)).start()
            return carry

        lax.fori_loop(0, RING - 1, one, 0)
        returned[0, stream] = result[stream, :, 0:9]

    for kind, stream, piece, detail in ORDER:
        if kind == PASS and piece == 0:
            begin(stream, detail)
        elif kind == PASS:
            pass_on(stream, piece, detail)
        else:
            if piece == 0:
                open_queries(stream)
            absorb(stream, piece, detail)
            if piece == PIECES - 1:
                finish(stream)

    for stream in range(STREAMS):
        await_bytes(returned.at[pl.ds(1, 7), stream], back_recv.at[stream])

        def unpack(k, carry):
            cols = columns_at(head_of(stream, k))
            for a, ref in enumerate((out_ref, out_tan_ref)):
                ref[0, 0:16, cols] = returned[k, stream, a, 0:8].reshape(16, HD)
                ref[0, 16:18, cols] = returned[k, stream, a, 8]
            return carry

        lax.fori_loop(0, RING, unpack, 0, unroll=4)

    await_bytes(packed.at[pl.ds(1, 7)], spread_send)
    await_bytes(result.at[:, :, pl.ds(9, 63)], back_send)
    for stream in range(STREAMS):
        await_bytes(
            store.at[stream, :, pl.ds(BLOCK, (2 * PIECES - 1) * BLOCK)],
            ring_send.at[stream],
        )


def local(*operands):
    operands = operands[:6] + tuple(g.reshape(1, HD) for g in operands[6:])
    shape = jax.ShapeDtypeStruct(operands[0].shape, jnp.bfloat16)
    vmem = pl.BlockSpec(memory_space=pltpu.VMEM)
    dma = pltpu.SemaphoreType.DMA
    bf16, f32 = jnp.bfloat16, jnp.float32
    out = pl.pallas_call(
        kernel,
        out_shape=(shape, shape),
        in_specs=[pl.BlockSpec(memory_space=pltpu.HBM)] * 8,
        out_specs=(vmem, vmem),
        scratch_shapes=[
            pltpu.VMEM((6, PART, operands[0].shape[2]), bf16),
            pltpu.VMEM((2, 1, HD), f32),
            pltpu.VMEM((RING, STREAMS, 6, 9, 2, HD), bf16),
            pltpu.VMEM((STREAMS, 6, 72, 2, HD), bf16),
            pltpu.VMEM((STREAMS, BLOCK, 2 * HD), bf16),
            pltpu.VMEM((STREAMS, 4, 2 * PIECES * BLOCK, HD), bf16),
            pltpu.VMEM((STREAMS, BLOCK, 1), f32),
            pltpu.VMEM((STREAMS, BLOCK, 1), f32),
            pltpu.VMEM((STREAMS, BLOCK, 1), f32),
            pltpu.VMEM((STREAMS, BLOCK, 2 * HD), f32),
            pltpu.VMEM((STREAMS, 2, 72, 2, HD), bf16),
            pltpu.VMEM((RING, STREAMS, 2, 9, 2, HD), bf16),
            dma((8,)),
            dma,
            dma((STREAMS, 3)),
            dma((STREAMS,)),
            dma((STREAMS, PIECES, 2)),
            dma((STREAMS, PIECES)),
            dma,
            dma((STREAMS,)),
        ],
        compiler_params=pltpu.CompilerParams(
            collective_id=0,
            has_side_effects=True,
            vmem_limit_bytes=40 * 1024 * 1024,
        ),
    )(*(pltpu.with_memory_space_constraint(a, pltpu.HBM) for a in operands))
    return out[0], out[1]


def solution(mesh):
    rows = P("blk", "head", None)
    return jax.shard_map(
        local,
        mesh=mesh,
        in_specs=(rows,) * 6 + (P(), P()),
        out_specs=(rows, rows),
        check_vma=False,
    )
```

```python
import math

import jax
import jax.numpy as jnp
from jax import lax
from jax.experimental import pallas as pl
from jax.experimental.pallas import tpu as pltpu
from jax.sharding import PartitionSpec as P

HD = 128
TXT = 512
GRID_W = 64
IMAGES = 4
RING = 8
PART = 18
BLOCK = RING * PART
STREAMS = 3
PIECES = 8
PASS, ABSORB = 0, 1
ORDER = (
    (PASS, 1, 0, 1), (PASS, 0, 0, 1), (PASS, 0, 0, 0), (PASS, 1, 0, 0), (PASS, 2, 0, 1),
    (ABSORB, 1, 0, 1), (PASS, 2, 0, 0), (PASS, 0, 1, 1), (PASS, 0, 2, 1), (PASS, 0, 1, 0),
    (PASS, 0, 2, 0), (ABSORB, 0, 0, 1), (PASS, 2, 2, 1), (ABSORB, 0, 1, 2), (PASS, 2, 1, 1),
    (PASS, 1, 2, 1), (PASS, 1, 1, 1), (ABSORB, 2, 0, 1), (PASS, 2, 1, 0), (PASS, 2, 2, 0),
    (PASS, 1, 2, 0), (PASS, 1, 1, 0), (PASS, 0, 4, 1), (PASS, 0, 3, 1), (ABSORB, 2, 1, 2),
    (PASS, 0, 4, 0), (PASS, 0, 3, 0), (PASS, 1, 4, 1), (PASS, 1, 3, 1), (ABSORB, 1, 1, 2),
    (PASS, 2, 3, 1), (PASS, 1, 4, 0), (PASS, 1, 3, 0), (ABSORB, 0, 3, 2), (PASS, 2, 4, 0),
    (PASS, 2, 3, 0), (PASS, 2, 4, 1), (ABSORB, 1, 3, 2), (PASS, 0, 5, 1), (PASS, 1, 6, 1),
    (PASS, 0, 6, 1), (PASS, 1, 5, 1), (ABSORB, 2, 3, 2), (PASS, 1, 6, 0), (PASS, 0, 5, 0),
    (PASS, 1, 5, 0), (PASS, 0, 6, 0), (PASS, 2, 6, 0), (PASS, 2, 5, 1), (ABSORB, 1, 5, 2),
    (PASS, 2, 6, 1), (PASS, 2, 5, 0), (PASS, 1, 7, 1), (ABSORB, 0, 5, 2), (PASS, 1, 7, 0),
    (ABSORB, 2, 5, 2), (PASS, 0, 7, 1), (PASS, 0, 7, 0), (ABSORB, 1, 7, 1), (PASS, 2, 7, 1),
    (PASS, 2, 7, 0), (ABSORB, 0, 7, 1), (ABSORB, 2, 7, 1),
)
NEAR = 80
TURN = (0, 1, 1)
QUERY, KEY, VALUE = 0, 1, 2

EPSILON = 1e-06
THETA = 10000.0
SCALE = 1.0 / math.sqrt(HD)
MESH = pl.DeviceIdType.MESH


def rows_at(slot):
    return pl.ds(slot * BLOCK, BLOCK)


def columns_at(head):
    return pl.ds(pl.multiple_of(head * HD, HD), HD)


def kernel(
    query_hbm,
    key_hbm,
    value_hbm,
    query_tan_hbm,
    key_tan_hbm,
    value_tan_hbm,
    query_gain_hbm,
    key_gain_hbm,
    out_ref,
    out_tan_ref,
    inputs,
    gains,
    packed,
    landed,
    queries,
    store,
    peak,
    total,
    drift,
    summed,
    result,
    returned,
    input_sem,
    spread_send,
    spread_recv,
    ring_send,
    ring_recv,
    partner_recv,
    back_send,
    back_recv,
):
    head = lax.axis_index("head")
    blk = lax.axis_index("blk")
    core = head % 2
    x = blk % IMAGES
    y = (head // 2) * 2 + (blk // IMAGES) % 2
    z = blk // (2 * IMAGES)

    def device(yy, zz, cc):
        return {"head": (yy // 2) * 2 + cc, "blk": (zz * 2 + yy % 2) * IMAGES + x}

    def spread(stream, hops):
        flip = stream % 2
        return device((y + hops * (1 - flip)) % RING, (z + hops * flip) % RING, core)

    def along(stream, hops):
        flip = stream % 2
        return device((y + hops * flip) % RING, (z + hops * (1 - flip)) % RING, core)

    partner = device(y, z, 1 - core)

    def head_of(stream, hops):
        if stream == 1:
            return 2 * RING + (z + hops) % RING
        return 2 * ((y + hops) % RING) + stream // 2

    barrier = pltpu.get_barrier_semaphore()

    def peer(i):
        return RING // 2 + (i + 1) // 2 * (1 - 2 * (i % 2))

    def greet(i, carry):
        k = peer(i)
        pl.semaphore_signal(barrier, inc=1, device_id=spread(0, k), device_id_type=MESH)
        pl.semaphore_signal(barrier, inc=1, device_id=spread(1, k), device_id_type=MESH)
        return carry

    lax.fori_loop(0, RING - 1, greet, 0)
    pl.semaphore_signal(barrier, inc=1, device_id=partner, device_id_type=MESH)

    sources = (query_hbm, query_tan_hbm, key_hbm, key_tan_hbm, value_hbm, value_tan_hbm)
    loads = [
        pltpu.make_async_copy(source.at[0], inputs.at[a], input_sem.at[a])
        for a, source in enumerate(sources)
    ]
    for i, source in enumerate((query_gain_hbm, key_gain_hbm)):
        loads.append(pltpu.make_async_copy(source, gains.at[i], input_sem.at[6 + i]))
    for a in (4, 5, 2, 3, 7, 0, 1, 6):
        loads[a].start()

    place = blk // IMAGES
    token = place * BLOCK + head * PART + lax.broadcasted_iota(jnp.int32, (PART, HD), 0)
    lane = lax.broadcasted_iota(jnp.int32, (PART, HD), 1)
    pair = lax.shift_right_logical(lane, 1)
    patch = jnp.maximum(token - TXT, 0)
    row_id = lax.shift_right_logical(patch, 6).astype(jnp.float32)
    column_id = (patch & (GRID_W - 1)).astype(jnp.float32)
    in_row = pair < 36
    step = jnp.where(in_row, pair - 8, pair - 36).astype(jnp.float32)
    frequency = jnp.exp(-math.log(THETA) * (step * (2.0 / 56)))
    angle = jnp.where(in_row, row_id, column_id) * frequency
    angle = jnp.where(pair < 8, 0.0, angle)
    odd = (lane & 1) == 1
    cosine = jnp.cos(angle)
    sine = jnp.sin(angle)
    sine = jnp.where(odd, sine, -sine)

    def rotate(v):
        swapped = jnp.where(odd, pltpu.roll(v, 1, 1), pltpu.roll(v, HD - 1, 1))
        return v * cosine + swapped * sine

    def normalize(raw, tangent, gain):
        values = raw.astype(jnp.float32)
        motion = tangent.astype(jnp.float32)
        inverse = lax.rsqrt(jnp.mean(values * values, axis=-1, keepdims=True) + EPSILON)
        coupling = jnp.mean(values * motion, axis=-1, keepdims=True)
        normed = values * inverse * gain
        normed_dot = gain * (
            motion * inverse - values * (inverse * inverse * inverse * coupling)
        )
        return rotate(normed).astype(jnp.bfloat16), rotate(normed_dot).astype(jnp.bfloat16)

    def put(k, stream, a, v):
        packed[k, stream, a, 0:8] = v[0:16].reshape(8, 2, HD)
        packed[k, stream, a, 8] = v[16:18]

    def pack(stream, group):
        def one(k, carry):
            cols = columns_at(head_of(stream, k))
            raw, tangent = inputs[2 * group, :, cols], inputs[2 * group + 1, :, cols]
            if group != VALUE:
                raw, tangent = normalize(raw, tangent, gains[group])
            put(k, stream, 2 * group, raw)
            put(k, stream, 2 * group + 1, tangent)
            return carry

        lax.fori_loop(0, RING, one, 0, unroll=4)
        pair = pl.ds(2 * group, 2)
        landed[stream, pair, 0:9] = packed[0, stream, pair]

    def spread_copy(stream, group, i):
        k = peer(i)
        pair = pl.ds(2 * group, 2)
        return pltpu.make_async_remote_copy(
            src_ref=packed.at[k, stream, pair],
            dst_ref=landed.at[stream, pair, pl.ds((RING - 1 - i) * 9, 9)],
            send_sem=spread_send,
            recv_sem=spread_recv.at[stream, group],
            device_id=spread(stream, k),
            device_id_type=MESH,
        )

    def send_out(stream, group):
        def one(i, carry):
            spread_copy(stream, group, i).start()
            return carry

        lax.fori_loop(0, RING - 1, one, 0)

    def await_bytes(ref, sem):
        pltpu.make_async_copy(ref, ref, sem).wait()

    for a in (4, 5):
        loads[a].wait()
    for stream in range(STREAMS):
        pack(stream, VALUE)
    for a in (2, 3, 7):
        loads[a].wait()
    for stream in (0, 1):
        pack(stream, KEY)
    pl.semaphore_wait(barrier, 2 * RING - 1)
    for group in (VALUE, KEY):
        for stream in (0, 1):
            send_out(stream, group)
    send_out(2, VALUE)
    pack(2, KEY)
    send_out(2, KEY)
    for a in (0, 1, 6):
        loads[a].wait()
    for stream in (1, 0, 2):
        pack(stream, QUERY)
        send_out(stream, QUERY)

    def ring_copy(stream, source, target, pair_of, to):
        pair = pl.ds(2 * pair_of, 2)
        return pltpu.make_async_remote_copy(
            src_ref=store.at[stream, pair, rows_at(source)],
            dst_ref=store.at[stream, pair, rows_at(target)],
            send_sem=ring_send.at[stream],
            recv_sem=ring_recv.at[stream, target // 2, pair_of],
            device_id=to,
            device_id_type=MESH,
        )

    def hand_over(stream, source, pair_of):
        pair = pl.ds(2 * pair_of, 2)
        return pltpu.make_async_remote_copy(
            src_ref=store.at[stream, pair, rows_at(source)],
            dst_ref=store.at[stream, pair, rows_at(source + 1)],
            send_sem=ring_send.at[stream],
            recv_sem=partner_recv.at[stream, source // 2],
            device_id=partner,
            device_id_type=MESH,
        )

    def await_spread(stream, group):
        await_bytes(
            landed.at[stream, pl.ds(2 * group, 2), pl.ds(9, 63)],
            spread_recv.at[stream, group],
        )

    def begin(stream, pair_of):
        await_spread(stream, pair_of + 1)
        for a in (2 * pair_of, 2 * pair_of + 1):
            store[stream, a, 0:BLOCK] = landed.at[stream, 2 + a].reshape(BLOCK, HD)[...]
        ring_copy(stream, 0, 2, pair_of, along(stream, 1)).start()
        ring_copy(stream, 0, 4, pair_of, along(stream, RING - 1)).start()
        hand_over(stream, 0, pair_of).start()

    def pass_on(stream, piece, pair_of):
        slot = 2 * piece
        await_bytes(
            store.at[stream, pl.ds(2 * pair_of, 2), rows_at(slot)],
            ring_recv.at[stream, piece, pair_of],
        )
        onward = along(stream, 1 if piece % 2 else RING - 1)
        if piece <= 4:
            ring_copy(stream, slot, slot + 4, pair_of, onward).start()
        elif piece == 5 + (pair_of ^ TURN[stream]):
            ring_copy(stream, slot, 14, pair_of, onward).start()
        hand_over(stream, slot, pair_of).start()

    def open_queries(stream):
        await_spread(stream, QUERY)
        query_hat = landed.at[stream, 0].reshape(BLOCK, HD)[...]
        query_dot = landed.at[stream, 1].reshape(BLOCK, HD)[...]
        queries[stream, :, 0:HD] = query_dot
        queries[stream, :, HD : 2 * HD] = query_hat
        peak[stream] = jnp.full((BLOCK, 1), -jnp.inf, jnp.float32)
        total[stream] = jnp.zeros((BLOCK, 1), jnp.float32)
        drift[stream] = jnp.zeros((BLOCK, 1), jnp.float32)
        summed[stream] = jnp.zeros((BLOCK, 2 * HD), jnp.float32)

    def absorb(stream, first_piece, count):
        for piece in range(first_piece, first_piece + count):
            await_bytes(
                store.at[stream, :, rows_at(2 * piece + 1)],
                partner_recv.at[stream, piece],
            )
        rows = pl.ds(first_piece * (2 * BLOCK), count * (2 * BLOCK))
        query_pair = queries[stream]
        query_hat = query_pair[:, HD:]
        key = store[stream, 0, rows]
        key_pair = jnp.concatenate([key, store[stream, 1, rows]], axis=1)
        value = store[stream, 2, rows]
        value_pair = jnp.concatenate([value, store[stream, 3, rows]], axis=1)
        contract = (((1,), (1,)), ((), ()))
        scores = (
            lax.dot_general(query_hat, key, contract, preferred_element_type=jnp.float32)
            * SCALE
        )
        scores_dot = (
            lax.dot_general(
                query_pair, key_pair, contract, preferred_element_type=jnp.float32
            )
            * SCALE
        )
        old_peak = peak[stream]
        new_peak = jnp.maximum(old_peak, jnp.max(scores, axis=1, keepdims=True))
        rescale = jnp.exp(old_peak - new_peak)
        weights = jnp.exp(scores - new_peak)
        product = weights * scores_dot
        peak[stream] = new_peak
        total[stream] = total[stream] * rescale + jnp.sum(weights, axis=1, keepdims=True)
        drift[stream] = drift[stream] * rescale + jnp.sum(product, axis=1, keepdims=True)
        low_weights = weights.astype(jnp.bfloat16)
        low_product = product.astype(jnp.bfloat16)
        first = jnp.dot(low_weights, value_pair, preferred_element_type=jnp.float32)
        second = jnp.dot(low_product, value, preferred_element_type=jnp.float32)
        summed[stream, :, 0:HD] = summed[stream, :, 0:HD] * rescale + first[:, 0:HD]
        summed[stream, :, HD:] = (
            summed[stream, :, HD:] * rescale + first[:, HD:] + second
        )

    def back_copy(stream, i):
        k = peer(i)
        return pltpu.make_async_remote_copy(
            src_ref=result.at[stream, :, pl.ds((RING - 1 - i) * 9, 9)],
            dst_ref=returned.at[k, stream],
            send_sem=back_send,
            recv_sem=back_recv.at[stream],
            device_id=spread(stream, RING - k),
            device_id_type=MESH,
        )

    def finish(stream):
        def one(i, carry):
            back_copy(stream, i).start()
            return carry

        for low, high, first, last in ((NEAR, BLOCK, 0, 3), (0, NEAR, 3, RING - 1)):
            inverse = 1.0 / total[stream, low:high]
            base = summed[stream, low:high, 0:HD]
            ratio = drift[stream, low:high] * inverse
            tangent = (summed[stream, low:high, HD:] - ratio * base) * inverse
            for a, v in enumerate((base * inverse, tangent)):
                rows = v.astype(jnp.bfloat16)
                result.at[stream, a].reshape(BLOCK, HD)[low:high] = rows
            lax.fori_loop(first, last, one, 0)
        returned[0, stream] = result[stream, :, 0:9]

    for kind, stream, piece, detail in ORDER:
        if kind == PASS and piece == 0:
            begin(stream, detail)
        elif kind == PASS:
            pass_on(stream, piece, detail)
        else:
            if piece == 0:
                open_queries(stream)
            absorb(stream, piece, detail)
            if piece == PIECES - 1:
                finish(stream)

    for stream in range(STREAMS):
        await_bytes(returned.at[pl.ds(1, 7), stream], back_recv.at[stream])

        def unpack(k, carry):
            cols = columns_at(head_of(stream, k))
            for a, ref in enumerate((out_ref, out_tan_ref)):
                ref[0, 0:16, cols] = returned[k, stream, a, 0:8].reshape(16, HD)
                ref[0, 16:18, cols] = returned[k, stream, a, 8]
            return carry

        lax.fori_loop(0, RING, unpack, 0, unroll=4)

    await_bytes(packed.at[pl.ds(1, 7)], spread_send)
    await_bytes(result.at[:, :, pl.ds(9, 63)], back_send)
    for stream in range(STREAMS):
        await_bytes(
            store.at[stream, :, pl.ds(BLOCK, (2 * PIECES - 1) * BLOCK)],
            ring_send.at[stream],
        )


def write_out(first, second, out_first, out_second, sems):
    copies = [
        pltpu.make_async_copy(source, target, sems.at[i])
        for i, (source, target) in enumerate(((first, out_first), (second, out_second)))
    ]
    for copy in copies:
        copy.start()
    for copy in copies:
        copy.wait()


def local(*operands):
    operands = operands[:6] + tuple(g.reshape(1, HD) for g in operands[6:])
    shape = jax.ShapeDtypeStruct(operands[0].shape, jnp.bfloat16)
    vmem = pl.BlockSpec(memory_space=pltpu.VMEM)
    dma = pltpu.SemaphoreType.DMA
    bf16, f32 = jnp.bfloat16, jnp.float32
    out = pl.pallas_call(
        kernel,
        out_shape=(shape, shape),
        in_specs=[pl.BlockSpec(memory_space=pltpu.HBM)] * 8,
        out_specs=(vmem, vmem),
        scratch_shapes=[
            pltpu.VMEM((6, PART, operands[0].shape[2]), bf16),
            pltpu.VMEM((2, 1, HD), f32),
            pltpu.VMEM((RING, STREAMS, 6, 9, 2, HD), bf16),
            pltpu.VMEM((STREAMS, 6, 72, 2, HD), bf16),
            pltpu.VMEM((STREAMS, BLOCK, 2 * HD), bf16),
            pltpu.VMEM((STREAMS, 4, 2 * PIECES * BLOCK, HD), bf16),
            pltpu.VMEM((STREAMS, BLOCK, 1), f32),
            pltpu.VMEM((STREAMS, BLOCK, 1), f32),
            pltpu.VMEM((STREAMS, BLOCK, 1), f32),
            pltpu.VMEM((STREAMS, BLOCK, 2 * HD), f32),
            pltpu.VMEM((STREAMS, 2, 72, 2, HD), bf16),
            pltpu.VMEM((RING, STREAMS, 2, 9, 2, HD), bf16),
            dma((8,)),
            dma,
            dma((STREAMS, 3)),
            dma((STREAMS,)),
            dma((STREAMS, PIECES, 2)),
            dma((STREAMS, PIECES)),
            dma,
            dma((STREAMS,)),
        ],
        compiler_params=pltpu.CompilerParams(
            collective_id=0,
            has_side_effects=True,
            vmem_limit_bytes=40 * 1024 * 1024,
        ),
    )(*(pltpu.with_memory_space_constraint(a, pltpu.HBM) for a in operands))
    hbm = pl.BlockSpec(memory_space=pltpu.HBM)
    return pl.pallas_call(
        write_out,
        out_shape=(shape, shape),
        in_specs=[vmem, vmem],
        out_specs=(hbm, hbm),
        scratch_shapes=[dma((2,))],
        compiler_params=pltpu.CompilerParams(vmem_limit_bytes=1024 * 1024),
    )(*(pltpu.with_memory_space_constraint(a, pltpu.VMEM) for a in out))


def solution(mesh):
    rows = P("blk", "head", None)
    return jax.shard_map(
        local,
        mesh=mesh,
        in_specs=(rows,) * 6 + (P(), P()),
        out_specs=(rows, rows),
        check_vma=False,
    )
```

```python
import math

import jax
import jax.numpy as jnp
from jax import lax
from jax.experimental import pallas as pl
from jax.experimental.pallas import tpu as pltpu
from jax.sharding import PartitionSpec as P

HD = 128
TXT = 512
GRID_W = 64
IMAGES = 4
RING = 8
PART = 18
BLOCK = RING * PART
STREAMS = 3
PIECES = 8
PASS, ABSORB = 0, 1
ORDER = (
    (PASS, 1, 0, 1), (PASS, 0, 0, 1), (PASS, 0, 0, 0), (PASS, 1, 0, 0), (PASS, 2, 0, 1),
    (ABSORB, 1, 0, 1), (PASS, 2, 0, 0), (PASS, 0, 1, 1), (PASS, 0, 2, 1), (PASS, 0, 1, 0),
    (PASS, 0, 2, 0), (ABSORB, 0, 0, 1), (PASS, 2, 2, 1), (ABSORB, 0, 1, 2), (PASS, 2, 1, 1),
    (PASS, 1, 2, 1), (PASS, 1, 1, 1), (ABSORB, 2, 0, 1), (PASS, 2, 1, 0), (PASS, 2, 2, 0),
    (PASS, 1, 2, 0), (PASS, 1, 1, 0), (PASS, 0, 4, 1), (PASS, 0, 3, 1), (ABSORB, 2, 1, 2),
    (PASS, 0, 4, 0), (PASS, 0, 3, 0), (PASS, 1, 4, 1), (PASS, 1, 3, 1), (ABSORB, 1, 1, 2),
    (PASS, 2, 3, 1), (PASS, 1, 4, 0), (PASS, 1, 3, 0), (ABSORB, 0, 3, 2), (PASS, 2, 4, 0),
    (PASS, 2, 3, 0), (PASS, 2, 4, 1), (ABSORB, 1, 3, 2), (PASS, 0, 5, 1), (PASS, 1, 6, 1),
    (PASS, 0, 6, 1), (PASS, 1, 5, 1), (ABSORB, 2, 3, 2), (PASS, 1, 6, 0), (PASS, 0, 5, 0),
    (PASS, 1, 5, 0), (PASS, 0, 6, 0), (PASS, 2, 6, 0), (PASS, 2, 5, 1), (ABSORB, 1, 5, 2),
    (PASS, 2, 6, 1), (PASS, 2, 5, 0), (PASS, 1, 7, 1), (ABSORB, 0, 5, 2), (PASS, 1, 7, 0),
    (PASS, 0, 7, 1), (PASS, 0, 7, 0), (ABSORB, 2, 5, 2), (PASS, 2, 7, 1), (PASS, 2, 7, 0),
    (ABSORB, 0, 7, 1), (ABSORB, 1, 7, 1), (ABSORB, 2, 7, 1),
)
OWN = 16
NEAR = 80
TURN = (0, 1, 1)
QUERY, KEY, VALUE = 0, 1, 2

EPSILON = 1e-06
THETA = 10000.0
SCALE = 1.0 / math.sqrt(HD)
MESH = pl.DeviceIdType.MESH


def rows_at(slot):
    return pl.ds(slot * BLOCK, BLOCK)


def columns_at(head):
    return pl.ds(pl.multiple_of(head * HD, HD), HD)


def kernel(
    query_hbm,
    key_hbm,
    value_hbm,
    query_tan_hbm,
    key_tan_hbm,
    value_tan_hbm,
    query_gain_hbm,
    key_gain_hbm,
    out_ref,
    out_tan_ref,
    inputs,
    gains,
    packed,
    landed,
    queries,
    store,
    peak,
    total,
    drift,
    summed,
    result,
    returned,
    input_sem,
    spread_send,
    spread_recv,
    ring_send,
    ring_recv,
    partner_recv,
    back_send,
    back_recv,
):
    head = lax.axis_index("head")
    blk = lax.axis_index("blk")
    core = head % 2
    x = blk % IMAGES
    y = (head // 2) * 2 + (blk // IMAGES) % 2
    z = blk // (2 * IMAGES)

    def device(yy, zz, cc):
        return {"head": (yy // 2) * 2 + cc, "blk": (zz * 2 + yy % 2) * IMAGES + x}

    def spread(stream, hops):
        flip = stream % 2
        return device((y + hops * (1 - flip)) % RING, (z + hops * flip) % RING, core)

    def along(stream, hops):
        flip = stream % 2
        return device((y + hops * flip) % RING, (z + hops * (1 - flip)) % RING, core)

    partner = device(y, z, 1 - core)

    def head_of(stream, hops):
        if stream == 1:
            return 2 * RING + (z + hops) % RING
        return 2 * ((y + hops) % RING) + stream // 2

    barrier = pltpu.get_barrier_semaphore()

    def peer(i):
        return RING // 2 + (i + 1) // 2 * (1 - 2 * (i % 2))

    def greet(i, carry):
        k = peer(i)
        pl.semaphore_signal(barrier, inc=1, device_id=spread(0, k), device_id_type=MESH)
        pl.semaphore_signal(barrier, inc=1, device_id=spread(1, k), device_id_type=MESH)
        return carry

    lax.fori_loop(0, RING - 1, greet, 0)
    pl.semaphore_signal(barrier, inc=1, device_id=partner, device_id_type=MESH)

    sources = (query_hbm, query_tan_hbm, key_hbm, key_tan_hbm, value_hbm, value_tan_hbm)
    loads = [
        pltpu.make_async_copy(source.at[0], inputs.at[a], input_sem.at[a])
        for a, source in enumerate(sources)
    ]
    for i, source in enumerate((query_gain_hbm, key_gain_hbm)):
        loads.append(pltpu.make_async_copy(source, gains.at[i], input_sem.at[6 + i]))
    for a in (4, 5, 2, 3, 7, 0, 1, 6):
        loads[a].start()

    place = blk // IMAGES
    token = place * BLOCK + head * PART + lax.broadcasted_iota(jnp.int32, (PART, HD), 0)
    lane = lax.broadcasted_iota(jnp.int32, (PART, HD), 1)
    pair = lax.shift_right_logical(lane, 1)
    patch = jnp.maximum(token - TXT, 0)
    row_id = lax.shift_right_logical(patch, 6).astype(jnp.float32)
    column_id = (patch & (GRID_W - 1)).astype(jnp.float32)
    in_row = pair < 36
    step = jnp.where(in_row, pair - 8, pair - 36).astype(jnp.float32)
    frequency = jnp.exp(-math.log(THETA) * (step * (2.0 / 56)))
    angle = jnp.where(in_row, row_id, column_id) * frequency
    angle = jnp.where(pair < 8, 0.0, angle)
    odd = (lane & 1) == 1
    cosine = jnp.cos(angle)
    sine = jnp.sin(angle)
    sine = jnp.where(odd, sine, -sine)

    def rotate(v):
        swapped = jnp.where(odd, pltpu.roll(v, 1, 1), pltpu.roll(v, HD - 1, 1))
        return v * cosine + swapped * sine

    def normalize(raw, tangent, gain):
        values = raw.astype(jnp.float32)
        motion = tangent.astype(jnp.float32)
        inverse = lax.rsqrt(jnp.mean(values * values, axis=-1, keepdims=True) + EPSILON)
        coupling = jnp.mean(values * motion, axis=-1, keepdims=True)
        normed = values * inverse * gain
        normed_dot = gain * (
            motion * inverse - values * (inverse * inverse * inverse * coupling)
        )
        return rotate(normed).astype(jnp.bfloat16), rotate(normed_dot).astype(jnp.bfloat16)

    def put(k, stream, a, v):
        packed[k, stream, a, 0:8] = v[0:16].reshape(8, 2, HD)
        packed[k, stream, a, 8] = v[16:18]

    def pack(stream, group):
        def one(k, carry):
            cols = columns_at(head_of(stream, k))
            raw, tangent = inputs[2 * group, :, cols], inputs[2 * group + 1, :, cols]
            if group != VALUE:
                raw, tangent = normalize(raw, tangent, gains[group])
            put(k, stream, 2 * group, raw)
            put(k, stream, 2 * group + 1, tangent)
            return carry

        lax.fori_loop(0, RING, one, 0, unroll=4)
        pair = pl.ds(2 * group, 2)
        landed[stream, pair, 0:9] = packed[0, stream, pair]

    def spread_copy(stream, group, i):
        k = peer(i)
        pair = pl.ds(2 * group, 2)
        return pltpu.make_async_remote_copy(
            src_ref=packed.at[k, stream, pair],
            dst_ref=landed.at[stream, pair, pl.ds((RING - 1 - i) * 9, 9)],
            send_sem=spread_send,
            recv_sem=spread_recv.at[stream, group],
            device_id=spread(stream, k),
            device_id_type=MESH,
        )

    def send_out(stream, group):
        def one(i, carry):
            spread_copy(stream, group, i).start()
            return carry

        lax.fori_loop(0, RING - 1, one, 0)

    def await_bytes(ref, sem):
        pltpu.make_async_copy(ref, ref, sem).wait()

    def ring_copy(stream, source, target, pair_of, to, low=0, high=BLOCK):
        pair = pl.ds(2 * pair_of, 2)
        return pltpu.make_async_remote_copy(
            src_ref=store.at[stream, pair, pl.ds(source * BLOCK + low, high - low)],
            dst_ref=store.at[stream, pair, pl.ds(target * BLOCK + low, high - low)],
            send_sem=ring_send.at[stream],
            recv_sem=ring_recv.at[stream, target // 2, pair_of],
            device_id=to,
            device_id_type=MESH,
        )

    def move_own(stream, pair_of, low, high):
        for a in (2 * pair_of, 2 * pair_of + 1):
            rows = landed.at[stream, 2 + a].reshape(BLOCK, HD)[low:high]
            store[stream, a, low:high] = rows

    def send_own(stream, pair_of, low, high):
        ring_copy(stream, 0, 2, pair_of, along(stream, 1), low, high).start()
        ring_copy(stream, 0, 4, pair_of, along(stream, RING - 1), low, high).start()

    for a in (4, 5):
        loads[a].wait()
    for stream in range(STREAMS):
        pack(stream, VALUE)
    for a in (2, 3, 7):
        loads[a].wait()
    for stream in (0, 1):
        pack(stream, KEY)
    for stream, pair_of in ((0, 1), (2, 1), (0, 0)):
        move_own(stream, pair_of, 0, OWN)
    pl.semaphore_wait(barrier, 2 * RING - 1)
    for group in (VALUE, KEY):
        for stream in (0, 1):
            send_out(stream, group)
    send_out(2, VALUE)
    for stream, pair_of in ((0, 1), (2, 1), (0, 0)):
        send_own(stream, pair_of, 0, OWN)
    pack(2, KEY)
    move_own(2, 0, 0, OWN)
    send_out(2, KEY)
    send_own(2, 0, 0, OWN)
    for a in (0, 1, 6):
        loads[a].wait()
    for stream in (1, 0, 2):
        pack(stream, QUERY)
        send_out(stream, QUERY)

    def hand_over(stream, source, pair_of):
        pair = pl.ds(2 * pair_of, 2)
        return pltpu.make_async_remote_copy(
            src_ref=store.at[stream, pair, rows_at(source)],
            dst_ref=store.at[stream, pair, rows_at(source + 1)],
            send_sem=ring_send.at[stream],
            recv_sem=partner_recv.at[stream, source // 2],
            device_id=partner,
            device_id_type=MESH,
        )

    def await_spread(stream, group):
        await_bytes(
            landed.at[stream, pl.ds(2 * group, 2), pl.ds(9, 63)],
            spread_recv.at[stream, group],
        )

    def begin(stream, pair_of):
        await_spread(stream, pair_of + 1)
        low = 0 if stream == 1 else OWN
        move_own(stream, pair_of, low, BLOCK)
        send_own(stream, pair_of, low, BLOCK)
        hand_over(stream, 0, pair_of).start()

    def pass_on(stream, piece, pair_of):
        slot = 2 * piece
        await_bytes(
            store.at[stream, pl.ds(2 * pair_of, 2), rows_at(slot)],
            ring_recv.at[stream, piece, pair_of],
        )
        onward = along(stream, 1 if piece % 2 else RING - 1)
        if piece <= 4:
            ring_copy(stream, slot, slot + 4, pair_of, onward).start()
        elif piece == 5 + (pair_of ^ TURN[stream]):
            ring_copy(stream, slot, 14, pair_of, onward).start()
        hand_over(stream, slot, pair_of).start()

    def open_queries(stream):
        await_spread(stream, QUERY)
        query_hat = landed.at[stream, 0].reshape(BLOCK, HD)[...]
        query_dot = landed.at[stream, 1].reshape(BLOCK, HD)[...]
        queries[stream, :, 0:HD] = query_dot
        queries[stream, :, HD : 2 * HD] = query_hat
        peak[stream] = jnp.full((BLOCK, 1), -jnp.inf, jnp.float32)
        total[stream] = jnp.zeros((BLOCK, 1), jnp.float32)
        drift[stream] = jnp.zeros((BLOCK, 1), jnp.float32)
        summed[stream] = jnp.zeros((BLOCK, 2 * HD), jnp.float32)

    def score(stream, first_piece, count):
        rows = pl.ds(first_piece * (2 * BLOCK), count * (2 * BLOCK))
        query_pair = queries[stream]
        key = store[stream, 0, rows]
        key_pair = jnp.concatenate([key, store[stream, 1, rows]], axis=1)
        contract = (((1,), (1,)), ((), ()))
        scores = lax.dot_general(
            query_pair[:, HD:], key, contract, preferred_element_type=jnp.float32
        )
        scores_dot = lax.dot_general(
            query_pair, key_pair, contract, preferred_element_type=jnp.float32
        )
        return scores * SCALE, scores_dot * SCALE

    def weigh(stream, scores, scores_dot):
        old_peak = peak[stream]
        new_peak = jnp.maximum(old_peak, jnp.max(scores, axis=1, keepdims=True))
        rescale = jnp.exp(old_peak - new_peak)
        weights = jnp.exp(scores - new_peak)
        product = weights * scores_dot
        peak[stream] = new_peak
        total[stream] = total[stream] * rescale + jnp.sum(weights, axis=1, keepdims=True)
        drift[stream] = drift[stream] * rescale + jnp.sum(product, axis=1, keepdims=True)
        return rescale, weights.astype(jnp.bfloat16), product.astype(jnp.bfloat16)

    def gather_values(stream, first_piece, count, rescale, low_weights, low_product):
        rows = pl.ds(first_piece * (2 * BLOCK), count * (2 * BLOCK))
        value = store[stream, 2, rows]
        value_pair = jnp.concatenate([value, store[stream, 3, rows]], axis=1)
        first = jnp.dot(low_weights, value_pair, preferred_element_type=jnp.float32)
        second = jnp.dot(low_product, value, preferred_element_type=jnp.float32)
        summed[stream, :, 0:HD] = summed[stream, :, 0:HD] * rescale + first[:, 0:HD]
        summed[stream, :, HD:] = (
            summed[stream, :, HD:] * rescale + first[:, HD:] + second
        )

    def absorb(units):
        for stream, first_piece, count in units:
            for piece in range(first_piece, first_piece + count):
                await_bytes(
                    store.at[stream, :, rows_at(2 * piece + 1)],
                    partner_recv.at[stream, piece],
                )
        scored = [score(*unit) for unit in units]
        weighed = [weigh(unit[0], *pair) for unit, pair in zip(units, scored)]
        for unit, parts in zip(units, weighed):
            gather_values(*unit, *parts)

    def back_copy(stream, i):
        k = peer(i)
        return pltpu.make_async_remote_copy(
            src_ref=result.at[stream, :, pl.ds((RING - 1 - i) * 9, 9)],
            dst_ref=returned.at[k, stream],
            send_sem=back_send,
            recv_sem=back_recv.at[stream],
            device_id=spread(stream, RING - k),
            device_id_type=MESH,
        )

    def finish(stream):
        for low, high, first, last in ((NEAR, BLOCK, 0, 3), (0, NEAR, 3, RING - 1)):
            inverse = 1.0 / total[stream, low:high]
            base = summed[stream, low:high, 0:HD]
            ratio = drift[stream, low:high] * inverse
            tangent = (summed[stream, low:high, HD:] - ratio * base) * inverse
            for a, v in enumerate((base * inverse, tangent)):
                rows = v.astype(jnp.bfloat16)
                result.at[stream, a].reshape(BLOCK, HD)[low:high] = rows
            for i in range(first, last):
                back_copy(stream, i).start()
        returned[0, stream] = result[stream, :, 0:9]

    for kind, *detail in ORDER:
        if kind == PASS and detail[1] == 0:
            begin(detail[0], detail[2])
        elif kind == PASS:
            pass_on(*detail)
        else:
            units = [tuple(detail[i : i + 3]) for i in range(0, len(detail), 3)]
            for stream, piece, _ in units:
                if piece == 0:
                    open_queries(stream)
            absorb(units)
            for stream, piece, _ in units:
                if piece == PIECES - 1:
                    finish(stream)

    for stream in range(STREAMS):
        await_bytes(returned.at[pl.ds(1, 7), stream], back_recv.at[stream])

        def unpack(k, carry):
            cols = columns_at(head_of(stream, k))
            for a, ref in enumerate((out_ref, out_tan_ref)):
                ref[0, 0:16, cols] = returned[k, stream, a, 0:8].reshape(16, HD)
                ref[0, 16:18, cols] = returned[k, stream, a, 8]
            return carry

        lax.fori_loop(0, RING, unpack, 0, unroll=4)

    await_bytes(packed.at[pl.ds(1, 7)], spread_send)
    await_bytes(result.at[:, :, pl.ds(9, 63)], back_send)
    for stream in range(STREAMS):
        await_bytes(
            store.at[stream, :, pl.ds(BLOCK, (2 * PIECES - 1) * BLOCK)],
            ring_send.at[stream],
        )


def write_out(first, second, out_first, out_second, sems):
    copies = [
        pltpu.make_async_copy(source, target, sems.at[i])
        for i, (source, target) in enumerate(((first, out_first), (second, out_second)))
    ]
    for copy in copies:
        copy.start()
    for copy in copies:
        copy.wait()


def local(*operands):
    operands = operands[:6] + tuple(g.reshape(1, HD) for g in operands[6:])
    shape = jax.ShapeDtypeStruct(operands[0].shape, jnp.bfloat16)
    vmem = pl.BlockSpec(memory_space=pltpu.VMEM)
    dma = pltpu.SemaphoreType.DMA
    bf16, f32 = jnp.bfloat16, jnp.float32
    out = pl.pallas_call(
        kernel,
        out_shape=(shape, shape),
        in_specs=[pl.BlockSpec(memory_space=pltpu.HBM)] * 8,
        out_specs=(vmem, vmem),
        scratch_shapes=[
            pltpu.VMEM((6, PART, operands[0].shape[2]), bf16),
            pltpu.VMEM((2, 1, HD), f32),
            pltpu.VMEM((RING, STREAMS, 6, 9, 2, HD), bf16),
            pltpu.VMEM((STREAMS, 6, 72, 2, HD), bf16),
            pltpu.VMEM((STREAMS, BLOCK, 2 * HD), bf16),
            pltpu.VMEM((STREAMS, 4, 2 * PIECES * BLOCK, HD), bf16),
            pltpu.VMEM((STREAMS, BLOCK, 1), f32),
            pltpu.VMEM((STREAMS, BLOCK, 1), f32),
            pltpu.VMEM((STREAMS, BLOCK, 1), f32),
            pltpu.VMEM((STREAMS, BLOCK, 2 * HD), f32),
            pltpu.VMEM((STREAMS, 2, 72, 2, HD), bf16),
            pltpu.VMEM((RING, STREAMS, 2, 9, 2, HD), bf16),
            dma((8,)),
            dma,
            dma((STREAMS, 3)),
            dma((STREAMS,)),
            dma((STREAMS, PIECES, 2)),
            dma((STREAMS, PIECES)),
            dma,
            dma((STREAMS,)),
        ],
        compiler_params=pltpu.CompilerParams(
            collective_id=0,
            has_side_effects=True,
            vmem_limit_bytes=40 * 1024 * 1024,
        ),
    )(*(pltpu.with_memory_space_constraint(a, pltpu.HBM) for a in operands))
    hbm = pl.BlockSpec(memory_space=pltpu.HBM)
    return pl.pallas_call(
        write_out,
        out_shape=(shape, shape),
        in_specs=[vmem, vmem],
        out_specs=(hbm, hbm),
        scratch_shapes=[dma((2,))],
        compiler_params=pltpu.CompilerParams(vmem_limit_bytes=1024 * 1024),
    )(*(pltpu.with_memory_space_constraint(a, pltpu.VMEM) for a in out))


def solution(mesh):
    rows = P("blk", "head", None)
    return jax.shard_map(
        local,
        mesh=mesh,
        in_specs=(rows,) * 6 + (P(), P()),
        out_specs=(rows, rows),
        check_vma=False,
    )
```

```python
import math

import jax
import jax.numpy as jnp
from jax import lax
from jax.experimental import pallas as pl
from jax.experimental.pallas import tpu as pltpu
from jax.sharding import PartitionSpec as P

HD = 128
TXT = 512
GRID_W = 64
IMAGES = 4
RING = 8
PART = 18
BLOCK = RING * PART
STREAMS = 3
PIECES = 8
PASS, ABSORB = 0, 1
ORDER = (
    (PASS, 1, 0, 1), (PASS, 0, 0, 1), (PASS, 0, 0, 0), (PASS, 1, 0, 0), (PASS, 2, 0, 1),
    (PASS, 0, 1, 1), (PASS, 0, 2, 1), (ABSORB, 1, 0, 1), (PASS, 2, 0, 0), (PASS, 0, 1, 0),
    (PASS, 0, 2, 0), (ABSORB, 0, 0, 1), (PASS, 2, 2, 1), (ABSORB, 0, 1, 2), (PASS, 2, 1, 1),
    (PASS, 1, 2, 1), (PASS, 1, 1, 1), (ABSORB, 2, 0, 1), (PASS, 2, 1, 0), (PASS, 2, 2, 0),
    (PASS, 1, 2, 0), (PASS, 1, 1, 0), (PASS, 0, 4, 1), (PASS, 0, 3, 1), (ABSORB, 2, 1, 2),
    (PASS, 0, 4, 0), (PASS, 0, 3, 0), (PASS, 1, 4, 1), (PASS, 1, 3, 1), (ABSORB, 1, 1, 2),
    (PASS, 2, 3, 1), (PASS, 1, 4, 0), (PASS, 1, 3, 0), (ABSORB, 0, 3, 2), (PASS, 2, 4, 0),
    (PASS, 2, 3, 0), (PASS, 2, 4, 1), (ABSORB, 1, 3, 2), (PASS, 0, 5, 1), (PASS, 1, 6, 1),
    (PASS, 0, 6, 1), (PASS, 1, 5, 1), (ABSORB, 2, 3, 2), (PASS, 1, 6, 0), (PASS, 0, 5, 0),
    (PASS, 1, 5, 0), (PASS, 0, 6, 0), (PASS, 2, 6, 0), (PASS, 2, 5, 1), (ABSORB, 1, 5, 2),
    (PASS, 2, 6, 1), (PASS, 2, 5, 0), (PASS, 1, 7, 1), (ABSORB, 0, 5, 2), (PASS, 1, 7, 0),
    (PASS, 0, 7, 1), (PASS, 0, 7, 0), (ABSORB, 2, 5, 2), (PASS, 2, 7, 1), (PASS, 2, 7, 0),
    (ABSORB, 0, 7, 1), (ABSORB, 1, 7, 1), (ABSORB, 2, 7, 1),
)
OWN = 16
NEAR = 80
TURN = (0, 1, 1)
QUERY, KEY, VALUE = 0, 1, 2

EPSILON = 1e-06
THETA = 10000.0
SCALE = 1.0 / math.sqrt(HD)
MESH = pl.DeviceIdType.MESH


def rows_at(slot):
    return pl.ds(slot * BLOCK, BLOCK)


def columns_at(head):
    return pl.ds(pl.multiple_of(head * HD, HD), HD)


def kernel(
    query_hbm,
    key_hbm,
    value_hbm,
    query_tan_hbm,
    key_tan_hbm,
    value_tan_hbm,
    query_gain_hbm,
    key_gain_hbm,
    out_ref,
    out_tan_ref,
    inputs,
    gains,
    packed,
    landed,
    queries,
    store,
    peak,
    total,
    drift,
    summed,
    result,
    returned,
    input_sem,
    spread_send,
    spread_recv,
    ring_send,
    ring_recv,
    partner_recv,
    back_send,
    back_recv,
):
    head = lax.axis_index("head")
    blk = lax.axis_index("blk")
    core = head % 2
    x = blk % IMAGES
    y = (head // 2) * 2 + (blk // IMAGES) % 2
    z = blk // (2 * IMAGES)

    def device(yy, zz, cc):
        return {"head": (yy // 2) * 2 + cc, "blk": (zz * 2 + yy % 2) * IMAGES + x}

    def spread(stream, hops):
        flip = stream % 2
        return device((y + hops * (1 - flip)) % RING, (z + hops * flip) % RING, core)

    def along(stream, hops):
        flip = stream % 2
        return device((y + hops * flip) % RING, (z + hops * (1 - flip)) % RING, core)

    partner = device(y, z, 1 - core)

    def head_of(stream, hops):
        if stream == 1:
            return 2 * RING + (z + hops) % RING
        return 2 * ((y + hops) % RING) + stream // 2

    barrier = pltpu.get_barrier_semaphore()

    def peer(i):
        return RING // 2 + (i + 1) // 2 * (1 - 2 * (i % 2))

    def greet(i, carry):
        k = peer(i)
        pl.semaphore_signal(barrier, inc=1, device_id=spread(0, k), device_id_type=MESH)
        pl.semaphore_signal(barrier, inc=1, device_id=spread(1, k), device_id_type=MESH)
        return carry

    lax.fori_loop(0, RING - 1, greet, 0)
    pl.semaphore_signal(barrier, inc=1, device_id=partner, device_id_type=MESH)

    sources = (query_hbm, query_tan_hbm, key_hbm, key_tan_hbm, value_hbm, value_tan_hbm)
    loads = [
        pltpu.make_async_copy(source.at[0], inputs.at[a], input_sem.at[a])
        for a, source in enumerate(sources)
    ]
    for i, source in enumerate((query_gain_hbm, key_gain_hbm)):
        loads.append(pltpu.make_async_copy(source, gains.at[i], input_sem.at[6 + i]))
    for a in (4, 5, 2, 3, 7, 0, 1, 6):
        loads[a].start()

    place = blk // IMAGES
    token = place * BLOCK + head * PART + lax.broadcasted_iota(jnp.int32, (PART, HD), 0)
    lane = lax.broadcasted_iota(jnp.int32, (PART, HD), 1)
    pair = lax.shift_right_logical(lane, 1)
    patch = jnp.maximum(token - TXT, 0)
    row_id = lax.shift_right_logical(patch, 6).astype(jnp.float32)
    column_id = (patch & (GRID_W - 1)).astype(jnp.float32)
    in_row = pair < 36
    step = jnp.where(in_row, pair - 8, pair - 36).astype(jnp.float32)
    frequency = jnp.exp(-math.log(THETA) * (step * (2.0 / 56)))
    angle = jnp.where(in_row, row_id, column_id) * frequency
    angle = jnp.where(pair < 8, 0.0, angle)
    odd = (lane & 1) == 1
    cosine = jnp.cos(angle)
    sine = jnp.sin(angle)
    sine = jnp.where(odd, sine, -sine)

    def rotate(v):
        swapped = jnp.where(odd, pltpu.roll(v, 1, 1), pltpu.roll(v, HD - 1, 1))
        return v * cosine + swapped * sine

    def normalize(raw, tangent, gain):
        values = raw.astype(jnp.float32)
        motion = tangent.astype(jnp.float32)
        inverse = lax.rsqrt(jnp.mean(values * values, axis=-1, keepdims=True) + EPSILON)
        coupling = jnp.mean(values * motion, axis=-1, keepdims=True)
        normed = values * inverse * gain
        normed_dot = gain * (
            motion * inverse - values * (inverse * inverse * inverse * coupling)
        )
        return rotate(normed).astype(jnp.bfloat16), rotate(normed_dot).astype(jnp.bfloat16)

    def put(k, stream, a, v):
        packed[k, stream, a, 0:8] = v[0:16].reshape(8, 2, HD)
        packed[k, stream, a, 8] = v[16:18]

    def pack(stream, group):
        def one(k, carry):
            cols = columns_at(head_of(stream, k))
            raw, tangent = inputs[2 * group, :, cols], inputs[2 * group + 1, :, cols]
            if group != VALUE:
                raw, tangent = normalize(raw, tangent, gains[group])
            put(k, stream, 2 * group, raw)
            put(k, stream, 2 * group + 1, tangent)
            return carry

        lax.fori_loop(0, RING, one, 0, unroll=4)
        pair = pl.ds(2 * group, 2)
        landed[stream, pair, 0:9] = packed[0, stream, pair]

    def spread_copy(stream, group, i):
        k = peer(i)
        pair = pl.ds(2 * group, 2)
        return pltpu.make_async_remote_copy(
            src_ref=packed.at[k, stream, pair],
            dst_ref=landed.at[stream, pair, pl.ds((RING - 1 - i) * 9, 9)],
            send_sem=spread_send,
            recv_sem=spread_recv.at[stream, group],
            device_id=spread(stream, k),
            device_id_type=MESH,
        )

    def send_out(stream, group):
        def one(i, carry):
            spread_copy(stream, group, i).start()
            return carry

        lax.fori_loop(0, RING - 1, one, 0)

    def await_bytes(ref, sem):
        pltpu.make_async_copy(ref, ref, sem).wait()

    def ring_copy(stream, source, target, pair_of, to, low=0, high=BLOCK):
        pair = pl.ds(2 * pair_of, 2)
        return pltpu.make_async_remote_copy(
            src_ref=store.at[stream, pair, pl.ds(source * BLOCK + low, high - low)],
            dst_ref=store.at[stream, pair, pl.ds(target * BLOCK + low, high - low)],
            send_sem=ring_send.at[stream],
            recv_sem=ring_recv.at[stream, target // 2, pair_of],
            device_id=to,
            device_id_type=MESH,
        )

    def move_own(stream, pair_of, low, high):
        for a in (2 * pair_of, 2 * pair_of + 1):
            rows = landed.at[stream, 2 + a].reshape(BLOCK, HD)[low:high]
            store[stream, a, low:high] = rows

    def send_own(stream, pair_of, low, high):
        ring_copy(stream, 0, 2, pair_of, along(stream, 1), low, high).start()
        ring_copy(stream, 0, 4, pair_of, along(stream, RING - 1), low, high).start()

    for a in (4, 5):
        loads[a].wait()
    for stream in range(STREAMS):
        pack(stream, VALUE)
    for a in (2, 3, 7):
        loads[a].wait()
    for stream in (0, 1):
        pack(stream, KEY)
    for stream, pair_of in ((0, 1), (2, 1), (0, 0)):
        move_own(stream, pair_of, 0, OWN)
    pl.semaphore_wait(barrier, 2 * RING - 1)
    for group in (VALUE, KEY):
        for stream in (0, 1):
            send_out(stream, group)
    send_out(2, VALUE)
    for stream, pair_of in ((0, 1), (2, 1), (0, 0)):
        send_own(stream, pair_of, 0, OWN)
    pack(2, KEY)
    move_own(2, 0, 0, OWN)
    send_out(2, KEY)
    send_own(2, 0, 0, OWN)
    for a in (0, 1, 6):
        loads[a].wait()
    for stream in (1, 0, 2):
        pack(stream, QUERY)
        send_out(stream, QUERY)

    def hand_over(stream, source, pair_of):
        pair = pl.ds(2 * pair_of, 2)
        return pltpu.make_async_remote_copy(
            src_ref=store.at[stream, pair, rows_at(source)],
            dst_ref=store.at[stream, pair, rows_at(source + 1)],
            send_sem=ring_send.at[stream],
            recv_sem=partner_recv.at[stream, source // 2],
            device_id=partner,
            device_id_type=MESH,
        )

    def await_spread(stream, group):
        await_bytes(
            landed.at[stream, pl.ds(2 * group, 2), pl.ds(9, 63)],
            spread_recv.at[stream, group],
        )

    def begin(stream, pair_of):
        await_spread(stream, pair_of + 1)
        low = 0 if stream == 1 else OWN
        move_own(stream, pair_of, low, BLOCK)
        send_own(stream, pair_of, low, BLOCK)
        hand_over(stream, 0, pair_of).start()

    def pass_on(stream, piece, pair_of):
        slot = 2 * piece
        await_bytes(
            store.at[stream, pl.ds(2 * pair_of, 2), rows_at(slot)],
            ring_recv.at[stream, piece, pair_of],
        )
        onward = along(stream, 1 if piece % 2 else RING - 1)
        if piece <= 4:
            ring_copy(stream, slot, slot + 4, pair_of, onward).start()
        elif piece == 5 + (pair_of ^ TURN[stream]):
            ring_copy(stream, slot, 14, pair_of, onward).start()
        hand_over(stream, slot, pair_of).start()

    def open_queries(stream):
        await_spread(stream, QUERY)
        query_hat = landed.at[stream, 0].reshape(BLOCK, HD)[...]
        query_dot = landed.at[stream, 1].reshape(BLOCK, HD)[...]
        queries[stream, :, 0:HD] = query_dot
        queries[stream, :, HD : 2 * HD] = query_hat
        peak[stream] = jnp.full((BLOCK, 1), -jnp.inf, jnp.float32)
        total[stream] = jnp.zeros((BLOCK, 1), jnp.float32)
        drift[stream] = jnp.zeros((BLOCK, 1), jnp.float32)
        summed[stream] = jnp.zeros((BLOCK, 2 * HD), jnp.float32)

    def score(stream, first_piece, count):
        rows = pl.ds(first_piece * (2 * BLOCK), count * (2 * BLOCK))
        query_pair = queries[stream]
        key = store[stream, 0, rows]
        key_pair = jnp.concatenate([key, store[stream, 1, rows]], axis=1)
        contract = (((1,), (1,)), ((), ()))
        scores = lax.dot_general(
            query_pair[:, HD:], key, contract, preferred_element_type=jnp.float32
        )
        scores_dot = lax.dot_general(
            query_pair, key_pair, contract, preferred_element_type=jnp.float32
        )
        return scores * SCALE, scores_dot * SCALE

    def weigh(stream, scores, scores_dot):
        old_peak = peak[stream]
        new_peak = jnp.maximum(old_peak, jnp.max(scores, axis=1, keepdims=True))
        rescale = jnp.exp(old_peak - new_peak)
        weights = jnp.exp(scores - new_peak)
        product = weights * scores_dot
        peak[stream] = new_peak
        total[stream] = total[stream] * rescale + jnp.sum(weights, axis=1, keepdims=True)
        drift[stream] = drift[stream] * rescale + jnp.sum(product, axis=1, keepdims=True)
        return rescale, weights.astype(jnp.bfloat16), product.astype(jnp.bfloat16)

    def gather_values(stream, first_piece, count, rescale, low_weights, low_product):
        rows = pl.ds(first_piece * (2 * BLOCK), count * (2 * BLOCK))
        value = store[stream, 2, rows]
        value_pair = jnp.concatenate([value, store[stream, 3, rows]], axis=1)
        first = jnp.dot(low_weights, value_pair, preferred_element_type=jnp.float32)
        second = jnp.dot(low_product, value, preferred_element_type=jnp.float32)
        summed[stream, :, 0:HD] = summed[stream, :, 0:HD] * rescale + first[:, 0:HD]
        summed[stream, :, HD:] = (
            summed[stream, :, HD:] * rescale + first[:, HD:] + second
        )

    def absorb(units):
        for stream, first_piece, count in units:
            for piece in range(first_piece, first_piece + count):
                await_bytes(
                    store.at[stream, :, rows_at(2 * piece + 1)],
                    partner_recv.at[stream, piece],
                )
        scored = [score(*unit) for unit in units]
        weighed = [weigh(unit[0], *pair) for unit, pair in zip(units, scored)]
        for unit, parts in zip(units, weighed):
            gather_values(*unit, *parts)

    def back_copy(stream, i):
        k = peer(i)
        return pltpu.make_async_remote_copy(
            src_ref=result.at[stream, :, pl.ds((RING - 1 - i) * 9, 9)],
            dst_ref=returned.at[k, stream],
            send_sem=back_send,
            recv_sem=back_recv.at[stream],
            device_id=spread(stream, RING - k),
            device_id_type=MESH,
        )

    def finish(stream):
        for low, high, first, last in ((NEAR, BLOCK, 0, 3), (0, NEAR, 3, RING - 1)):
            inverse = 1.0 / total[stream, low:high]
            base = summed[stream, low:high, 0:HD]
            ratio = drift[stream, low:high] * inverse
            tangent = (summed[stream, low:high, HD:] - ratio * base) * inverse
            for a, v in enumerate((base * inverse, tangent)):
                rows = v.astype(jnp.bfloat16)
                result.at[stream, a].reshape(BLOCK, HD)[low:high] = rows
            for i in range(first, last):
                back_copy(stream, i).start()
        returned[0, stream] = result[stream, :, 0:9]

    for kind, *detail in ORDER:
        if kind == PASS and detail[1] == 0:
            begin(detail[0], detail[2])
        elif kind == PASS:
            pass_on(*detail)
        else:
            units = [tuple(detail[i : i + 3]) for i in range(0, len(detail), 3)]
            for stream, piece, _ in units:
                if piece == 0:
                    open_queries(stream)
            absorb(units)
            for stream, piece, _ in units:
                if piece == PIECES - 1:
                    finish(stream)

    for stream in range(STREAMS):
        await_bytes(returned.at[pl.ds(1, 7), stream], back_recv.at[stream])

        def unpack(k, carry):
            cols = columns_at(head_of(stream, k))
            for a, ref in enumerate((out_ref, out_tan_ref)):
                ref[0, 0:16, cols] = returned[k, stream, a, 0:8].reshape(16, HD)
                ref[0, 16:18, cols] = returned[k, stream, a, 8]
            return carry

        lax.fori_loop(0, RING, unpack, 0, unroll=4)

    await_bytes(packed.at[pl.ds(1, 7)], spread_send)
    await_bytes(result.at[:, :, pl.ds(9, 63)], back_send)
    for stream in range(STREAMS):
        await_bytes(
            store.at[stream, :, pl.ds(BLOCK, (2 * PIECES - 1) * BLOCK)],
            ring_send.at[stream],
        )


def write_out(first, second, out_first, out_second, sems):
    copies = [
        pltpu.make_async_copy(source, target, sems.at[i])
        for i, (source, target) in enumerate(((first, out_first), (second, out_second)))
    ]
    for copy in copies:
        copy.start()
    for copy in copies:
        copy.wait()


def local(*operands):
    operands = operands[:6] + tuple(g.reshape(1, HD) for g in operands[6:])
    shape = jax.ShapeDtypeStruct(operands[0].shape, jnp.bfloat16)
    vmem = pl.BlockSpec(memory_space=pltpu.VMEM)
    dma = pltpu.SemaphoreType.DMA
    bf16, f32 = jnp.bfloat16, jnp.float32
    out = pl.pallas_call(
        kernel,
        out_shape=(shape, shape),
        in_specs=[pl.BlockSpec(memory_space=pltpu.HBM)] * 8,
        out_specs=(vmem, vmem),
        scratch_shapes=[
            pltpu.VMEM((6, PART, operands[0].shape[2]), bf16),
            pltpu.VMEM((2, 1, HD), f32),
            pltpu.VMEM((RING, STREAMS, 6, 9, 2, HD), bf16),
            pltpu.VMEM((STREAMS, 6, 72, 2, HD), bf16),
            pltpu.VMEM((STREAMS, BLOCK, 2 * HD), bf16),
            pltpu.VMEM((STREAMS, 4, 2 * PIECES * BLOCK, HD), bf16),
            pltpu.VMEM((STREAMS, BLOCK, 1), f32),
            pltpu.VMEM((STREAMS, BLOCK, 1), f32),
            pltpu.VMEM((STREAMS, BLOCK, 1), f32),
            pltpu.VMEM((STREAMS, BLOCK, 2 * HD), f32),
            pltpu.VMEM((STREAMS, 2, 72, 2, HD), bf16),
            pltpu.VMEM((RING, STREAMS, 2, 9, 2, HD), bf16),
            dma((8,)),
            dma,
            dma((STREAMS, 3)),
            dma((STREAMS,)),
            dma((STREAMS, PIECES, 2)),
            dma((STREAMS, PIECES)),
            dma,
            dma((STREAMS,)),
        ],
        compiler_params=pltpu.CompilerParams(
            collective_id=0,
            has_side_effects=True,
            vmem_limit_bytes=40 * 1024 * 1024,
        ),
    )(*(pltpu.with_memory_space_constraint(a, pltpu.HBM) for a in operands))
    hbm = pl.BlockSpec(memory_space=pltpu.HBM)
    return pl.pallas_call(
        write_out,
        out_shape=(shape, shape),
        in_specs=[vmem, vmem],
        out_specs=(hbm, hbm),
        scratch_shapes=[dma((2,))],
        compiler_params=pltpu.CompilerParams(vmem_limit_bytes=1024 * 1024),
    )(*(pltpu.with_memory_space_constraint(a, pltpu.VMEM) for a in out))


def solution(mesh):
    rows = P("blk", "head", None)
    return jax.shard_map(
        local,
        mesh=mesh,
        in_specs=(rows,) * 6 + (P(), P()),
        out_specs=(rows, rows),
        check_vma=False,
    )
```
